256 devices in a mesh: grid: 64 (over z, x, core), band: 4 (over y).
Axes of the slice: x: 4, y: 4, z: 8, core: 2. Of those that a mesh axis runs over, the one named last changes fastest.
Arguments:
- basis: float32 [2048, 65536], P('band', 'grid'), as said below
- panel: float32 [1024, 65536], P('band', 'grid'), may hold values from -6 to 6
Outputs:
- new_panel: float32 [1024, 65536], P('band', 'grid')
- coeffs: float32 [2048, 1024], P('band')
The draws below stay inside these ranges and needn't reach their ends.
Inputs may be any that keep to these rules, and one draw needn't show every extreme that they name: The rows of basis are orthogonal to each other, each with squared sum 65536 (to float32 rounding).
All inputs are finite; a program needn't handle non-finite values.
Results may differ from the reference program's by a relative error of at most 0.000073.
Values sent between devices are 32-bit elements; how exact they have to be, the bound alone decides.
A program may use at most 128 MiB of HBM per device.

```python
import jax
import jax.numpy as jnp
from jax import lax

NQ = 2048
NP = 1024
NG = 65536


def draw_basis(key, part):
    sample = jax.random.normal(key, (NG, NQ), jnp.float32)
    ortho, upper = jnp.linalg.qr(sample)
    return (ortho.T * jnp.sqrt(jnp.float32(NG))).astype(jnp.float32)


def shard_levels(key, dims, split, least, high):
    def one(axis_at, blocks):
        steps = jax.random.uniform(jax.random.fold_in(jax.random.fold_in(key, 6), axis_at), (blocks,), jnp.float32, least / len(split), high / len(split))
        return jnp.repeat(jnp.exp(steps), dims[axis_at] // blocks).reshape((-1,) + (1,) * (len(dims) - axis_at - 1))

    loudness = one(*split[0])
    for cut in split[1:]:
        loudness = loudness * one(*cut)
    return loudness


def noise(key, shape, width, bound, shards=(), kind=jnp.bfloat16):
    array = jax.random.normal(key, shape, jnp.float32) * width
    if len(shards) > 0:
        array = shard_levels(key, shape, shards, -0.22, 0.18) * array
    return jnp.clip(array, min=-bound, max=bound).astype(kind)


def setup_inputs(seed: int = 0) -> dict:
    key_list = jax.random.split(jax.random.key(seed), 3)
    basis = draw_basis(jax.random.fold_in(key_list[2], 71), 0)
    panel = noise(key_list[1], (NP, NG), 1.0, 6.0, ((0, 4), (1, 64)), jnp.float32)
    return dict(basis=basis, panel=panel)


def reference(basis, panel):
    highest = lax.Precision.HIGHEST
    n_grid = basis.shape[1]
    coeffs = jnp.dot(basis, panel.T, precision=highest) / n_grid
    projected = panel - jnp.dot(coeffs.T, basis, precision=highest)
    gram = jnp.dot(projected, projected.T, precision=highest) / n_grid
    factor = jnp.linalg.cholesky(gram)
    new_panel = lax.linalg.triangular_solve(factor, projected, left_side=True, lower=True)
    return (new_panel, coeffs)
```

```python
import jax
import jax.numpy as jnp
from jax import lax
from jax.experimental import pallas as pl
from jax.experimental.pallas import tpu as pltpu
from jax.sharding import PartitionSpec as P

F32, BF16 = jnp.float32, jnp.bfloat16

def halves(x):
    hi = x.astype(BF16)
    return hi, (x - hi.astype(F32)).astype(BF16)

def dot3(a, b, dims):
    (ah, al), (bh, bl) = a, b
    dg = lambda u, v: lax.dot_general(u, v, (dims, ((), ())), preferred_element_type=F32)
    return dg(ah, bh) + (dg(ah, bl) + dg(al, bh))

NN, TN, NT = ((1,), (0,)), ((0,), (0,)), ((1,), (1,))
BASE = 32

def base_block(w, at):
    n = w.shape[0]
    rows = w[at:at + BASE]
    lane = lax.broadcasted_iota(jnp.int32, (BASE, n), 1)
    sub = lax.broadcasted_iota(jnp.int32, (BASE, n), 0)
    cols = []
    for j in range(BASE):
        lo = j // 8 * 8
        cols.append(jnp.broadcast_to(rows[lo:, at + j:at + j + 1], (BASE - lo, n)))
    inside = (lane >= at) & (lane < at + BASE)
    v = jnp.where(inside, (lane == sub + at).astype(F32), rows)
    v = [v[8 * s:8 * s + 8] for s in range(BASE // 8)]
    cols = [[c[8 * s:8 * s + 8] for s in range(c.shape[0] // 8)] for c in cols]
    nb = BASE // 8
    sub8 = lax.broadcasted_iota(jnp.int32, (8, n), 0)
    bc = lambda x, i: jnp.broadcast_to(x[i:i + 1], (8, n))
    for j in range(BASE):
        s0, r0 = j // 8, j % 8
        c = cols[j]
        inv = lax.rsqrt(bc(c[0], r0))
        l = [x * inv for x in c]
        for jj in range(j + 1, BASE):
            s1, r1 = jj // 8, jj % 8
            f = bc(l[s1 - s0], r1)
            for s in range(s1, nb):
                cols[jj][s - s1] = cols[jj][s - s1] - l[s - s0] * f
        piv = bc(v[s0], r0) * inv
        l0 = jnp.where(sub8 > r0, l[0], 0.0)
        v[s0] = jnp.where(sub8 == r0, piv, v[s0] - l0 * piv)
        for s in range(s0 + 1, nb):
            v[s] = v[s] - l[s - s0] * piv
    return jnp.concatenate(v, 0)

def factor128(w):
    n = w.shape[0]
    lane = lax.broadcasted_iota(jnp.int32, (n, n), 1)
    row = lax.broadcasted_iota(jnp.int32, (n, n), 0)
    for at in range(0, n, BASE):
        v = base_block(w, at)
        end = at + BASE
        if end < n:
            parts = halves(v)
            upd = lax.dot_general(v, v, (TN, ((), ())), precision=lax.Precision.HIGHEST, preferred_element_type=F32)
            below = w[end:]
            l2 = lane[end:]
            below = jnp.where((l2 >= at) & (l2 < end), 0.0, below) - upd[end:]
            w = jnp.concatenate(([w[:at]] if at else []) + [v, below], 0)
        else:
            w = jnp.concatenate([w[:at], v], 0)
    return jnp.where(lane <= row, w, 0.0)

B = 128

def chol_kernel(g_ref, m_ref, th, tl):
    n = g_ref.shape[0]
    nb = n // B
    m_ref[...] = g_ref[...]

    def step(k, _):
        r = pl.multiple_of(k * B, B)
        inv = factor128(m_ref[pl.ds(r, B), pl.ds(r, B)])
        t = dot3(halves(inv), halves(m_ref[pl.ds(r, B), :]), NN)
        m_ref[pl.ds(r, B), :] = t
        m_ref[pl.ds(r, B), pl.ds(r, B)] = inv
        hi, lo = halves(m_ref[pl.ds(r, B), :])
        th[...] = hi
        tl[...] = lo

        def rest(i, _):
            q = pl.multiple_of(i * B, B)
            m_ref[pl.ds(q, B), pl.ds(r, B)] = jnp.zeros((B, B), F32)
            f = (th[:, pl.ds(q, B)], tl[:, pl.ds(q, B)])
            m_ref[pl.ds(q, B), :] = m_ref[pl.ds(q, B), :] - dot3(f, (th[...], tl[...]), TN)
            return 0
        lax.fori_loop(k + 1, nb, rest, 0)
        return 0
    lax.fori_loop(0, nb, step, 0)

def inverse_factor(g):
    n = g.shape[0]
    return pl.pallas_call(
        chol_kernel,
        out_shape=jax.ShapeDtypeStruct((n, n), F32),
        in_specs=[pl.BlockSpec(memory_space=pltpu.VMEM)],
        out_specs=pl.BlockSpec(memory_space=pltpu.VMEM),
        scratch_shapes=[pltpu.VMEM((B, n), BF16), pltpu.VMEM((B, n), BF16)],
        compiler_params=pltpu.CompilerParams(vmem_limit_bytes=40 * 2**20),
    )(g)


def together(arrays, axis):
    ravelled, at, finished = (jnp.concatenate([a.reshape(-1) for a in arrays]), 0, [])
    total = lax.psum(ravelled, axis)
    for a in arrays:
        finished.append(total[at : at + a.size].reshape(a.shape))
        at += a.size
    return tuple(finished)


def cut_along(array, dim, count):
    before, after = (array.shape[:dim], array.shape[dim + 1 :])
    return jnp.moveaxis(array.reshape(*before, count, -1, *after), dim, 0)


def summed_on_arrival(array, axis, dim):
    blocks = cut_along(array, dim, lax.axis_size(axis))
    arrived = lax.all_to_all(blocks, axis, split_axis=0, concat_axis=0, tiled=True)
    return arrived.sum(axis=0)


def tdot(left, right):
    return lax.dot_general(
        left,
        right,
        (((1,), (1,)), ((), ())),
        precision=lax.Precision.HIGH,
        preferred_element_type=jnp.float32,
    )


def ndot(left, right):
    return jnp.dot(left, right, precision=lax.Precision.HIGH)


def body(basis, panel):
    n_grid = panel.shape[1] * lax.axis_size("grid")
    n_band = lax.axis_size("band")
    rows_q = basis.shape[0]
    rows_p = panel.shape[0]
    n_panel = rows_p * n_band
    stacked = jnp.concatenate([basis, panel], 0)
    both = tdot(stacked, lax.all_gather(panel, "band", axis=0, tiled=True))
    coeff_sum, gram_sum = together((both[:rows_q], both[rows_q:]), "grid")
    coeffs = coeff_sum / n_grid
    projected = panel - lax.psum_scatter(
        ndot(coeffs.T, basis), "band", scatter_dimension=0, tiled=True
    )
    gram_part = gram_sum / n_grid - summed_on_arrival(ndot(coeffs.T, coeffs), "band", 0)
    gram = lax.all_gather(gram_part, "band", axis=0, tiled=True)
    offset = lax.axis_index("band") * rows_p
    inverse_rows = lax.dynamic_slice_in_dim(inverse_factor(gram), offset, rows_p, 0)
    row_ids = lax.broadcasted_iota(jnp.int32, (rows_p, n_panel), 0)
    col_ids = lax.broadcasted_iota(jnp.int32, (rows_p, n_panel), 1)
    inverse_rows = jnp.where(col_ids <= row_ids + offset, inverse_rows, 0.0)
    new_panel = ndot(inverse_rows, lax.all_gather(projected, "band", axis=0, tiled=True))
    return (new_panel, coeffs)


def solution(mesh):
    placed = (P("band", "grid"), P("band", "grid"))
    return jax.shard_map(
        body,
        mesh=mesh,
        in_specs=placed,
        out_specs=(P("band", "grid"), P("band", None)),
        check_vma=False,
    )
```

```python
import jax
import jax.numpy as jnp
from jax import lax
from jax.experimental import pallas as pl
from jax.experimental.pallas import tpu as pltpu
from jax.sharding import PartitionSpec as P

F32, BF16 = jnp.float32, jnp.bfloat16

def halves(x):
    hi = x.astype(BF16)
    return hi, (x - hi.astype(F32)).astype(BF16)

def dot3(a, b, dims):
    (ah, al), (bh, bl) = a, b
    dg = lambda u, v: lax.dot_general(u, v, (dims, ((), ())), preferred_element_type=F32)
    return dg(ah, bh) + (dg(ah, bl) + dg(al, bh))

NN, TN, NT = ((1,), (0,)), ((0,), (0,)), ((1,), (1,))
BASE = 32

def base_block(w, at):
    n = w.shape[0]
    rows = w[at:at + BASE]
    lane = lax.broadcasted_iota(jnp.int32, (BASE, n), 1)
    sub = lax.broadcasted_iota(jnp.int32, (BASE, n), 0)
    cols = []
    for j in range(BASE):
        lo = j // 8 * 8
        cols.append(jnp.broadcast_to(rows[lo:, at + j:at + j + 1], (BASE - lo, n)))
    inside = (lane >= at) & (lane < at + BASE)
    v = jnp.where(inside, (lane == sub + at).astype(F32), rows)
    v = [v[8 * s:8 * s + 8] for s in range(BASE // 8)]
    cols = [[c[8 * s:8 * s + 8] for s in range(c.shape[0] // 8)] for c in cols]
    nb = BASE // 8
    sub8 = lax.broadcasted_iota(jnp.int32, (8, n), 0)
    bc = lambda x, i: jnp.broadcast_to(x[i:i + 1], (8, n))
    for j in range(BASE):
        s0, r0 = j // 8, j % 8
        c = cols[j]
        inv = lax.rsqrt(bc(c[0], r0))
        l = [x * inv for x in c]
        for jj in range(j + 1, BASE):
            s1, r1 = jj // 8, jj % 8
            f = bc(l[s1 - s0], r1)
            for s in range(s1, nb):
                cols[jj][s - s1] = cols[jj][s - s1] - l[s - s0] * f
        piv = bc(v[s0], r0) * inv
        l0 = jnp.where(sub8 > r0, l[0], 0.0)
        v[s0] = jnp.where(sub8 == r0, piv, v[s0] - l0 * piv)
        for s in range(s0 + 1, nb):
            v[s] = v[s] - l[s - s0] * piv
    return jnp.concatenate(v, 0)

def factor128(w):
    n = w.shape[0]
    lane = lax.broadcasted_iota(jnp.int32, (n, n), 1)
    row = lax.broadcasted_iota(jnp.int32, (n, n), 0)
    for at in range(0, n, BASE):
        v = base_block(w, at)
        end = at + BASE
        if end < n:
            parts = halves(v)
            upd = lax.dot_general(v, v, (TN, ((), ())), precision=lax.Precision.HIGHEST, preferred_element_type=F32)
            below = w[end:]
            l2 = lane[end:]
            below = jnp.where((l2 >= at) & (l2 < end), 0.0, below) - upd[end:]
            w = jnp.concatenate(([w[:at]] if at else []) + [v, below], 0)
        else:
            w = jnp.concatenate([w[:at], v], 0)
    return jnp.where(lane <= row, w, 0.0)

B = 128


def chol_kernel(g_ref, m_ref, th, tl):
    n = m_ref.shape[0]
    nb = n // B
    hb = g_ref.shape[0] // 2
    for t in range(nb // 2):
        for c in range(2):
            src = pl.ds(c * hb + t * 64, 64)
            m_ref[pl.ds(t * B + c * 64, 64), pl.ds(t * B, n - t * B)] = g_ref[src, pl.ds(0, n - t * B)]
            u = nb - 1 - t
            m_ref[pl.ds(u * B + c * 64, 64), pl.ds(u * B, n - u * B)] = g_ref[src, pl.ds(n - t * B, n - u * B)]

    def step(k, _):
        r = pl.multiple_of(k * B, B)
        inv = factor128(m_ref[pl.ds(r, B), pl.ds(r, B)])
        t = dot3(halves(inv), halves(m_ref[pl.ds(r, B), :]), NN)
        m_ref[pl.ds(r, B), :] = t
        m_ref[pl.ds(r, B), pl.ds(r, B)] = inv
        hi, lo = halves(m_ref[pl.ds(r, B), :])
        th[...] = hi
        tl[...] = lo

        def rest(i, _):
            q = pl.multiple_of(i * B, B)
            m_ref[pl.ds(q, B), pl.ds(r, B)] = jnp.zeros((B, B), F32)
            f = (th[:, pl.ds(q, B)], tl[:, pl.ds(q, B)])
            m_ref[pl.ds(q, B), :] = m_ref[pl.ds(q, B), :] - dot3(f, (th[...], tl[...]), TN)
            return 0
        lax.fori_loop(k + 1, nb, rest, 0)
        return 0
    lax.fori_loop(0, nb, step, 0)
    for t in range(nb - 1):
        m_ref[pl.ds(t * B, B), pl.ds(t * B + B, n - t * B - B)] = jnp.zeros((B, n - t * B - B), F32)


def inverse_factor(g, n):
    return pl.pallas_call(
        chol_kernel,
        name="inverse_factor",
        out_shape=jax.ShapeDtypeStruct((n, n), F32),
        in_specs=[pl.BlockSpec(memory_space=pltpu.VMEM)],
        out_specs=pl.BlockSpec(memory_space=pltpu.VMEM),
        scratch_shapes=[pltpu.VMEM((B, n), BF16), pltpu.VMEM((B, n), BF16)],
        compiler_params=pltpu.CompilerParams(vmem_limit_bytes=40 * 2**20),
    )(g)


MESH = pl.DeviceIdType.MESH
NX, NZ, NY = 4, 8, 4


def place():
    g = lax.axis_index("grid")
    return lax.rem(g, 2), lax.rem(lax.div(g, 2), NX), lax.div(g, 2 * NX), lax.axis_index("band")


def grid_id(z, x, c):
    return {"grid": (z * NX + x) * 2 + c}


def sender(send, recv):
    made = []

    def copy(src, dst, device):
        at = len(made)
        made.append(
            pltpu.make_async_remote_copy(
                src_ref=src, dst_ref=dst, send_sem=send.at[at], recv_sem=recv.at[at],
                device_id=device, device_id_type=MESH,
            )
        )
        made[-1].start()
        return made[-1]

    return copy, made


def greet(devices):
    barrier = pltpu.get_barrier_semaphore()
    for device in devices:
        pl.semaphore_signal(barrier, inc=1, device_id=device, device_id_type=MESH)
    pl.semaphore_wait(barrier, len(devices))


def rows_of(start, count):
    return pl.ds(pl.multiple_of(start, 8), count)


def lanes_of(start, count):
    return pl.ds(pl.multiple_of(start, 128), count)


def communicate(kernel, name, out_shape, operands, scratch, copies, cid):
    space = pl.BlockSpec(memory_space=pltpu.VMEM)
    return pl.pallas_call(
        kernel,
        name=name,
        out_shape=jax.ShapeDtypeStruct(out_shape, F32),
        in_specs=[space] * len(operands),
        out_specs=space,
        scratch_shapes=[pltpu.VMEM(s, F32) for s in scratch]
        + [pltpu.SemaphoreType.DMA((copies,)), pltpu.SemaphoreType.DMA((copies,))],
        compiler_params=pltpu.CompilerParams(
            collective_id=cid, has_side_effects=True, vmem_limit_bytes=48 * 2**20
        ),
    )(*operands)


def ring_gather(copy, out, base, count, mine, right, left, wrap, size):
    half = count // 2
    first = lambda q: out.at[rows_of(base + q * count, half)]
    second = lambda q: out.at[rows_of(base + q * count + half, half)]
    a = copy(first(mine), first(mine), right)
    b = copy(second(mine), second(mine), left)
    c = copy(second(mine), second(mine), right)
    d = copy(first(mine), first(mine), left)
    before, after, far = wrap(mine + size - 1), wrap(mine + 1), wrap(mine + 2)
    a.wait_recv()
    e = copy(first(before), first(before), right)
    b.wait_recv()
    f = copy(second(after), second(after), left)
    c.wait_recv()
    yield before
    d.wait_recv()
    yield after
    e.wait_recv()
    f.wait_recv()
    yield far


def gather_kernel(p_ref, out, send, recv):
    _, _, _, y = place()
    n = p_ref.shape[0]
    half = n // 2
    wrap = lambda q: lax.rem(q, NY)
    right, left = {"band": wrap(y + 1)}, {"band": wrap(y + NY - 1)}
    greet([right, left])
    copy, made = sender(send, recv)
    first = lambda q: out.at[rows_of(q * n, half)]
    second = lambda q: out.at[rows_of(q * n + half, half)]
    p1, p2 = p_ref.at[pl.ds(0, half)], p_ref.at[pl.ds(half, half)]
    a = copy(p1, first(y), right)
    b = copy(p2, second(y), left)
    c = copy(p2, second(y), right)
    d = copy(p1, first(y), left)
    out[rows_of(y * n, n)] = p_ref[...]
    a.wait_recv()
    e = copy(first(wrap(y + NY - 1)), first(wrap(y + NY - 1)), right)
    b.wait_recv()
    f = copy(second(wrap(y + 1)), second(wrap(y + 1)), left)
    for m in (c, d, e, f):
        m.wait_recv()
    for m in made:
        m.wait_send()


def gather_band(p):
    n, w = p.shape
    return communicate(gather_kernel, "gather_band", (n * NY, w), [p], [], 6, 1)


def scatter_kernel(z_ref, base, out, mid, send, recv):
    _, _, _, y = place()
    n = base.shape[0]
    half = n // 2
    wrap = lambda q: lax.rem(q, NY)
    right, left = {"band": wrap(y + 1)}, {"band": wrap(y + NY - 1)}
    before, after, far = wrap(y + NY - 1), wrap(y + 1), wrap(y + 2)
    greet([right, left])
    copy, made = sender(send, recv)
    first = lambda q: rows_of(q * n, half)
    second = lambda q: rows_of(q * n + half, half)
    a = copy(z_ref.at[first(far)], mid.at[0], right)
    b = copy(z_ref.at[second(far)], mid.at[1], left)
    c = copy(z_ref.at[second(after)], mid.at[2], right)
    d = copy(z_ref.at[first(before)], mid.at[3], left)
    a.wait_recv()
    mid[6] = mid[0] + z_ref[first(after)]
    e = copy(mid.at[6], mid.at[4], right)
    b.wait_recv()
    mid[7] = mid[1] + z_ref[second(before)]
    f = copy(mid.at[7], mid.at[5], left)
    c.wait_recv()
    d.wait_recv()
    e.wait_recv()
    out[pl.ds(0, half)] = base[pl.ds(0, half)] - (z_ref[first(y)] + (mid[3] + mid[4]))
    f.wait_recv()
    out[pl.ds(half, half)] = base[pl.ds(half, half)] - (z_ref[second(y)] + (mid[2] + mid[5]))
    for m in made:
        m.wait_send()


def subtract_scattered(z, base):
    n, w = base.shape
    return communicate(scatter_kernel, "scatter_band", (n, w), [z, base], [(8, n // 2, w)], 6, 2)


def total_kernel(v, out, pair, acc, ring, bz, bx, bfin, bcol, az, afin, send, recv):
    c, x, z, _ = place()
    half = v.shape[0] // 2
    nb = bcol.shape[0]
    na = half - nb
    pa, pb = na // NX, nb // NX
    h = pa // 2
    wx, wz = (lambda q: lax.rem(q, NX)), (lambda q: lax.rem(q, NZ))
    other = grid_id(z, x, 1 - c)
    right, left = grid_id(z, wx(x + 1), c), grid_id(z, wx(x + NX - 1), c)
    xs = [grid_id(z, wx(x + d), c) for d in range(1, NX)]
    zs = [grid_id(wz(z + d), x, c) for d in range(1, NZ)]
    greet([other] + xs + zs)
    copy, made = sender(send, recv)
    mine, theirs = c * half, (1 - c) * half
    B = pl.ds(na, nb)
    A = pl.ds(0, na)
    sb = copy(v.at[rows_of(theirs + na, nb)], pair.at[B], other)
    sa = copy(v.at[rows_of(theirs, na)], pair.at[A], other)
    sb.wait_recv()
    acc[B] = v[rows_of(mine + na, nb)] + pair[B]
    b1 = [copy(acc.at[B, lanes_of(wz(z + d) * 128, 128)], bz.at[d - 1], zs[d - 1]) for d in range(1, NZ)]
    sa.wait_recv()
    acc[A] = v[rows_of(mine, na)] + pair[A]
    up = lambda q: rows_of(q * pa, h)
    down = lambda q: rows_of(q * pa + h, h)
    before, after, far = wx(x + NX - 1), wx(x + 1), wx(x + 2)
    m0 = copy(acc.at[up(far)], ring.at[0], right)
    m1 = copy(acc.at[down(far)], ring.at[1], left)
    m2 = copy(acc.at[down(after)], ring.at[2], right)
    m3 = copy(acc.at[up(before)], ring.at[3], left)
    m0.wait_recv()
    ring[6] = acc[up(after)] + ring[0]
    m4 = copy(ring.at[6], ring.at[4], right)
    m1.wait_recv()
    ring[7] = acc[down(before)] + ring[1]
    m5 = copy(ring.at[7], ring.at[5], left)
    for m in b1:
        m.wait_recv()
    t = acc[B, lanes_of(z * 128, 128)]
    for d in range(NZ - 1):
        t = t + bz[d]
    bfin[...] = t
    b2 = [copy(bfin.at[rows_of(wx(x + d) * pb, pb)], bx.at[d - 1], xs[d - 1]) for d in range(1, NX)]
    for m in (m2, m3, m4, m5):
        m.wait_recv()
    acc[up(x)] = acc[up(x)] + (ring[3] + ring[4])
    acc[down(x)] = acc[down(x)] + (ring[2] + ring[5])
    piece = rows_of(x * pa, pa)
    a1 = [copy(acc.at[piece, lanes_of(wz(z + d) * 128, 128)], az.at[d - 1], zs[d - 1]) for d in range(1, NZ)]
    for m in b2:
        m.wait_recv()
    bq = rows_of(x * pb, pb)
    s = bfin[bq, :]
    for d in range(NX - 1):
        s = s + bx[d]
    bcol[bq, :] = s
    b3 = [copy(bcol.at[bq], bcol.at[bq], xs[d - 1]) for d in range(1, NX)]
    for m in a1:
        m.wait_recv()
    t = acc[piece, lanes_of(z * 128, 128)]
    for d in range(NZ - 1):
        t = t + az[d]
    afin[...] = t
    cols = lanes_of(z * 128, 128)
    a2 = [copy(afin, out.at[rows_of(mine + x * pa, pa), cols], zs[d - 1]) for d in range(1, NZ)]
    out[rows_of(mine + x * pa, pa), cols] = t
    for m in b3:
        m.wait_recv()
    ob = rows_of(mine + na, nb)
    b4 = [copy(bcol, out.at[ob, cols], zs[d - 1]) for d in range(1, NZ)]
    out[ob, cols] = bcol[...]
    for m in a2:
        m.wait_recv()
    last = []
    whole = lambda q: out.at[rows_of(mine + q * pa, pa)]
    parts = ring_gather(copy, out, mine, pa, x, right, left, wx, NX)
    got = next(parts)
    last.append(copy(whole(x), whole(x), other))
    last.append(copy(whole(got), whole(got), other))
    got = next(parts)
    last.append(copy(whole(got), whole(got), other))
    for m in b4:
        m.wait_recv()
    last.append(copy(out.at[ob], out.at[ob], other))
    got = next(parts)
    last.append(copy(whole(got), whole(got), other))
    for m in last:
        m.wait_recv()
    for m in made:
        m.wait_send()


def total_grid(v):
    n, w = v.shape
    half = n // 2
    nb = 64
    pa = (half - nb) // NX
    scratch = [
        (half, w), (half, w), (8, pa // 2, w), (NZ - 1, nb, 128), (NX - 1, nb // NX, 128),
        (nb, 128), (nb, 128), (NZ - 1, pa, 128), (pa, 128),
    ]
    return communicate(total_kernel, "total_grid", (n, w), [v], scratch, 2 + 7 + 6 + 3 + 7 + 3 + 7 + 7 + 6 + 5, 3)


def gram_kernel(part, out, yb, fin, send, recv):
    c, x, z, y = place()
    n = part.shape[0]
    q = n // NY
    wx, wy = (lambda q: lax.rem(q, NX)), (lambda q: lax.rem(q, NY))
    other = grid_id(z, x, 1 - c)
    xs = [grid_id(z, wx(x + d), c) for d in range(1, NX)]
    ys = [{"band": wy(y + d)} for d in range(1, NY)]
    greet([other, xs[0], xs[2]] + ys)
    copy, made = sender(send, recv)
    r1 = [copy(part.at[rows_of(wy(y + d) * q, q)], yb.at[d - 1], ys[d - 1]) for d in range(1, NY)]
    for m in r1:
        m.wait_recv()
    t = part[rows_of(y * q, q)]
    for d in range(NY - 1):
        t = t + yb[d]
    fin[...] = t
    base = c * (n * NX)
    at = rows_of(base + x * n + y * q, q)
    r2 = [copy(fin, out.at[at], ys[d - 1]) for d in range(1, NY)]
    out[at] = t
    for m in r2:
        m.wait_recv()
    whole = lambda b: out.at[rows_of(base + b * n, n)]
    last = []
    parts = ring_gather(copy, out, base, n, x, xs[0], xs[2], wx, NX)
    got = next(parts)
    last.append(copy(whole(x), whole(x), other))
    last.append(copy(whole(got), whole(got), other))
    for got in parts:
        last.append(copy(whole(got), whole(got), other))
    for m in last:
        m.wait_recv()
    for m in made:
        m.wait_send()


def total_gram(part):
    n, w = part.shape
    return communicate(gram_kernel, "total_gram", (2 * NX * n, w), [part], [(NY - 1, n // NY, w), (n // NY, w)], 3 + 3 + 6 + 4, 4)


def part_kernel(cf, pp, out, ch, cl, tmp):
    c, x, _, y = place()
    ch[...], cl[...] = halves(cf[...])
    for s in range(9):
        upper = s < 8 - x
        rb = jnp.where(upper, x, 7 - x)
        cb = jnp.where(upper, x + s, s - 1)
        r, q = lanes_of(rb * 128, 128), lanes_of(cb * 128, 128)
        prod = dot3((ch[:, r], cl[:, r]), (ch[:, q], cl[:, q]), TN)
        own = (lax.div(rb, 2) == y).astype(F32)
        tmp[...] = own * pp[rows_of(lax.rem(rb, 2) * 128, 128), q] - prod
        out[:, pl.ds(s * 128, 128)] = tmp[rows_of(c * 64, 64), :]


def gram_part(cf, pp):
    space = pl.BlockSpec(memory_space=pltpu.VMEM)
    return pl.pallas_call(
        part_kernel,
        name="gram_part",
        out_shape=jax.ShapeDtypeStruct((64, 9 * 128), F32),
        in_specs=[space] * 2,
        out_specs=space,
        scratch_shapes=[pltpu.VMEM(cf.shape, BF16), pltpu.VMEM(cf.shape, BF16), pltpu.VMEM((128, 128), F32)],
    )(cf, pp)


def tdot(left, right):
    return lax.dot_general(left, right, (NT, ((), ())), precision=lax.Precision.HIGH, preferred_element_type=F32)


def ndot(left, right):
    return jnp.dot(left, right, precision=lax.Precision.HIGH)


def body(basis, panel):
    n_grid = panel.shape[1] * lax.axis_size("grid")
    rows_q, rows_p = basis.shape[0], panel.shape[0]
    n_panel = rows_p * lax.axis_size("band")
    whole = gather_band(panel)
    both = total_grid(tdot(jnp.concatenate([basis, panel], 0), whole))
    coeffs = both[:rows_q] / n_grid
    gram = total_gram(gram_part(coeffs, both[rows_q:] / n_grid))
    inverse = inverse_factor(gram, n_panel)
    outer = ndot(tdot(inverse, coeffs), basis)
    rows = lax.dynamic_slice_in_dim(inverse, lax.axis_index("band") * rows_p, rows_p, 0)
    new_panel = subtract_scattered(outer, ndot(rows, whole))
    return (new_panel, coeffs)


def solution(mesh):
    placed = (P("band", "grid"), P("band", "grid"))
    return jax.shard_map(
        body, mesh=mesh, in_specs=placed, out_specs=(P("band", "grid"), P("band", None)), check_vma=False,
    )
```

```python
import functools

import jax
import jax.numpy as jnp
from jax import lax
from jax.experimental import pallas as pl
from jax.experimental.pallas import tpu as pltpu
from jax.sharding import PartitionSpec as P

F32, BF16 = jnp.float32, jnp.bfloat16

def halves(x):
    hi = x.astype(BF16)
    return hi, (x - hi.astype(F32)).astype(BF16)

def dot3(a, b, dims):
    (ah, al), (bh, bl) = a, b
    dg = lambda u, v: lax.dot_general(u, v, (dims, ((), ())), preferred_element_type=F32)
    return dg(ah, bh) + (dg(ah, bl) + dg(al, bh))

NN, TN, NT = ((1,), (0,)), ((0,), (0,)), ((1,), (1,))
BASE = 32

def base_block(w, at):
    n = w.shape[0]
    rows = w[at:at + BASE]
    lane = lax.broadcasted_iota(jnp.int32, (BASE, n), 1)
    sub = lax.broadcasted_iota(jnp.int32, (BASE, n), 0)
    cols = []
    for j in range(BASE):
        lo = j // 8 * 8
        cols.append(jnp.broadcast_to(rows[lo:, at + j:at + j + 1], (BASE - lo, n)))
    inside = (lane >= at) & (lane < at + BASE)
    v = jnp.where(inside, (lane == sub + at).astype(F32), rows)
    v = [v[8 * s:8 * s + 8] for s in range(BASE // 8)]
    cols = [[c[8 * s:8 * s + 8] for s in range(c.shape[0] // 8)] for c in cols]
    nb = BASE // 8
    sub8 = lax.broadcasted_iota(jnp.int32, (8, n), 0)
    bc = lambda x, i: jnp.broadcast_to(x[i:i + 1], (8, n))
    for j in range(BASE):
        s0, r0 = j // 8, j % 8
        c = cols[j]
        inv = lax.rsqrt(bc(c[0], r0))
        l = [x * inv for x in c]
        for jj in range(j + 1, BASE):
            s1, r1 = jj // 8, jj % 8
            f = bc(l[s1 - s0], r1)
            for s in range(s1, nb):
                cols[jj][s - s1] = cols[jj][s - s1] - l[s - s0] * f
        piv = bc(v[s0], r0) * inv
        l0 = jnp.where(sub8 > r0, l[0], 0.0)
        v[s0] = jnp.where(sub8 == r0, piv, v[s0] - l0 * piv)
        for s in range(s0 + 1, nb):
            v[s] = v[s] - l[s - s0] * piv
    return jnp.concatenate(v, 0)

def factor128(w):
    n = w.shape[0]
    lane = lax.broadcasted_iota(jnp.int32, (n, n), 1)
    row = lax.broadcasted_iota(jnp.int32, (n, n), 0)
    for at in range(0, n, BASE):
        v = base_block(w, at)
        end = at + BASE
        if end < n:
            parts = halves(v)
            upd = lax.dot_general(v, v, (TN, ((), ())), precision=lax.Precision.HIGHEST, preferred_element_type=F32)
            below = w[end:]
            l2 = lane[end:]
            below = jnp.where((l2 >= at) & (l2 < end), 0.0, below) - upd[end:]
            w = jnp.concatenate(([w[:at]] if at else []) + [v, below], 0)
        else:
            w = jnp.concatenate([w[:at], v], 0)
    return jnp.where(lane <= row, w, 0.0)

B = 128


SCATTERED_AT, PASSED_AT = 3, 6


def factorize(g_ref, m_ref, th, tl, between):
    n = m_ref.shape[0]
    nb = n // B
    hb = g_ref.shape[0] // 2
    for t in range(nb // 2):
        for c in range(2):
            src = pl.ds(c * hb + t * 64, 64)
            m_ref[pl.ds(t * B + c * 64, 64), pl.ds(t * B, n - t * B)] = g_ref[src, pl.ds(0, n - t * B)]
            u = nb - 1 - t
            m_ref[pl.ds(u * B + c * 64, 64), pl.ds(u * B, n - u * B)] = g_ref[src, pl.ds(n - t * B, n - u * B)]

    def step(k, _):
        r = pl.multiple_of(k * B, B)
        inv = factor128(m_ref[pl.ds(r, B), pl.ds(r, B)])
        t = dot3(halves(inv), halves(m_ref[pl.ds(r, B), :]), NN)
        m_ref[pl.ds(r, B), :] = t
        m_ref[pl.ds(r, B), pl.ds(r, B)] = inv
        hi, lo = halves(m_ref[pl.ds(r, B), :])
        th[...] = hi
        tl[...] = lo

        def rest(i, _):
            q = pl.multiple_of(i * B, B)
            m_ref[pl.ds(q, B), pl.ds(r, B)] = jnp.zeros((B, B), F32)
            f = (th[:, pl.ds(q, B)], tl[:, pl.ds(q, B)])
            m_ref[pl.ds(q, B), :] = m_ref[pl.ds(q, B), :] - dot3(f, (th[...], tl[...]), TN)
            return 0
        lax.fori_loop(k + 1, nb, rest, 0)
        for when, act in between.items():
            pl.when(k == when)(act)
        return 0
    lax.fori_loop(0, nb, step, 0)
    for t in range(nb - 1):
        m_ref[pl.ds(t * B, B), pl.ds(t * B + B, n - t * B - B)] = jnp.zeros((B, n - t * B - B), F32)


MESH = pl.DeviceIdType.MESH
NX, NZ, NY = 4, 8, 4


def place():
    g = lax.axis_index("grid")
    return lax.rem(g, 2), lax.rem(lax.div(g, 2), NX), lax.div(g, 2 * NX), lax.axis_index("band")


def grid_id(z, x, c):
    return {"grid": (z * NX + x) * 2 + c}


def sender(send, recv):
    made = []

    def copy(src, dst, device):
        at = len(made)
        made.append(
            pltpu.make_async_remote_copy(
                src_ref=src, dst_ref=dst, send_sem=send.at[at], recv_sem=recv.at[at],
                device_id=device, device_id_type=MESH,
            )
        )
        made[-1].start()
        return made[-1]

    return copy, made


def greet(devices):
    barrier = pltpu.get_barrier_semaphore()
    for device in devices:
        pl.semaphore_signal(barrier, inc=1, device_id=device, device_id_type=MESH)
    pl.semaphore_wait(barrier, len(devices))


def rows_of(start, count):
    return pl.ds(pl.multiple_of(start, 8), count)


def lanes_of(start, count):
    return pl.ds(pl.multiple_of(start, 128), count)


def communicate(kernel, name, out_shape, operands, scratch, copies, cid):
    space = pl.BlockSpec(memory_space=pltpu.VMEM)
    return pl.pallas_call(
        kernel,
        name=name,
        out_shape=jax.ShapeDtypeStruct(out_shape, F32),
        in_specs=[space] * len(operands),
        out_specs=space,
        scratch_shapes=[pltpu.VMEM(s, F32) for s in scratch]
        + [pltpu.SemaphoreType.DMA((copies,)), pltpu.SemaphoreType.DMA((copies,))],
        compiler_params=pltpu.CompilerParams(
            collective_id=cid, has_side_effects=True, vmem_limit_bytes=48 * 2**20
        ),
    )(*operands)


def ring_gather(copy, out, base, count, mine, right, left, wrap, size):
    half = count // 2
    first = lambda q: out.at[rows_of(base + q * count, half)]
    second = lambda q: out.at[rows_of(base + q * count + half, half)]
    a = copy(first(mine), first(mine), right)
    b = copy(second(mine), second(mine), left)
    c = copy(second(mine), second(mine), right)
    d = copy(first(mine), first(mine), left)
    before, after, far = wrap(mine + size - 1), wrap(mine + 1), wrap(mine + 2)
    a.wait_recv()
    e = copy(first(before), first(before), right)
    b.wait_recv()
    f = copy(second(after), second(after), left)
    c.wait_recv()
    yield before
    d.wait_recv()
    yield after
    e.wait_recv()
    f.wait_recv()
    yield far


def gather_kernel(p_ref, out, send, recv):
    _, _, _, y = place()
    n = p_ref.shape[0]
    half = n // 2
    wrap = lambda q: lax.rem(q, NY)
    right, left = {"band": wrap(y + 1)}, {"band": wrap(y + NY - 1)}
    greet([right, left])
    copy, made = sender(send, recv)
    first = lambda q: out.at[rows_of(q * n, half)]
    second = lambda q: out.at[rows_of(q * n + half, half)]
    p1, p2 = p_ref.at[pl.ds(0, half)], p_ref.at[pl.ds(half, half)]
    a = copy(p1, first(y), right)
    b = copy(p2, second(y), left)
    c = copy(p2, second(y), right)
    d = copy(p1, first(y), left)
    out[rows_of(y * n, n)] = p_ref[...]
    a.wait_recv()
    e = copy(first(wrap(y + NY - 1)), first(wrap(y + NY - 1)), right)
    b.wait_recv()
    f = copy(second(wrap(y + 1)), second(wrap(y + 1)), left)
    for m in (c, d, e, f):
        m.wait_recv()
    for m in made:
        m.wait_send()


def gather_band(p):
    n, w = p.shape
    return communicate(gather_kernel, "gather_band", (n * NY, w), [p], [], 6, 1)


def total_kernel(scale, v, out, pair, acc, ring, bz, bx, bfin, bcol, az, afin, send, recv):
    c, x, z, _ = place()
    half = v.shape[0] // 2
    nb = bcol.shape[0]
    na = half - nb
    pa, pb = na // NX, nb // NX
    h = pa // 2
    wx, wz = (lambda q: lax.rem(q, NX)), (lambda q: lax.rem(q, NZ))
    other = grid_id(z, x, 1 - c)
    right, left = grid_id(z, wx(x + 1), c), grid_id(z, wx(x + NX - 1), c)
    xs = [grid_id(z, wx(x + d), c) for d in range(1, NX)]
    zs = [grid_id(wz(z + d), x, c) for d in range(1, NZ)]
    greet([other] + xs + zs)
    copy, made = sender(send, recv)
    mine, theirs = c * half, (1 - c) * half
    B = pl.ds(na, nb)
    A = pl.ds(0, na)
    sb = copy(v.at[rows_of(theirs + na, nb)], pair.at[B], other)
    sa = copy(v.at[rows_of(theirs, na)], pair.at[A], other)
    sb.wait_recv()
    acc[B] = v[rows_of(mine + na, nb)] + pair[B]
    b1 = [copy(acc.at[B, lanes_of(wz(z + d) * 128, 128)], bz.at[d - 1], zs[d - 1]) for d in range(1, NZ)]
    sa.wait_recv()
    acc[A] = v[rows_of(mine, na)] + pair[A]
    up = lambda q: rows_of(q * pa, h)
    down = lambda q: rows_of(q * pa + h, h)
    before, after, far = wx(x + NX - 1), wx(x + 1), wx(x + 2)
    m0 = copy(acc.at[up(far)], ring.at[0], right)
    m1 = copy(acc.at[down(far)], ring.at[1], left)
    m2 = copy(acc.at[down(after)], ring.at[2], right)
    m3 = copy(acc.at[up(before)], ring.at[3], left)
    m0.wait_recv()
    ring[6] = acc[up(after)] + ring[0]
    m4 = copy(ring.at[6], ring.at[4], right)
    m1.wait_recv()
    ring[7] = acc[down(before)] + ring[1]
    m5 = copy(ring.at[7], ring.at[5], left)
    for m in b1:
        m.wait_recv()
    t = acc[B, lanes_of(z * 128, 128)]
    for d in range(NZ - 1):
        t = t + bz[d]
    bfin[...] = t
    b2 = [copy(bfin.at[rows_of(wx(x + d) * pb, pb)], bx.at[d - 1], xs[d - 1]) for d in range(1, NX)]
    for m in (m2, m3, m4, m5):
        m.wait_recv()
    acc[up(x)] = acc[up(x)] + (ring[3] + ring[4])
    acc[down(x)] = acc[down(x)] + (ring[2] + ring[5])
    piece = rows_of(x * pa, pa)
    a1 = [copy(acc.at[piece, lanes_of(wz(z + d) * 128, 128)], az.at[d - 1], zs[d - 1]) for d in range(1, NZ)]
    for m in b2:
        m.wait_recv()
    bq = rows_of(x * pb, pb)
    s = bfin[bq, :]
    for d in range(NX - 1):
        s = s + bx[d]
    bcol[bq, :] = s * scale
    b3 = [copy(bcol.at[bq], bcol.at[bq], xs[d - 1]) for d in range(1, NX)]
    for m in a1:
        m.wait_recv()
    t = acc[piece, lanes_of(z * 128, 128)]
    for d in range(NZ - 1):
        t = t + az[d]
    t = t * scale
    afin[...] = t
    cols = lanes_of(z * 128, 128)
    a2 = [copy(afin, out.at[rows_of(mine + x * pa, pa), cols], zs[d - 1]) for d in range(1, NZ)]
    out[rows_of(mine + x * pa, pa), cols] = t
    for m in b3:
        m.wait_recv()
    ob = rows_of(mine + na, nb)
    b4 = [copy(bcol, out.at[ob, cols], zs[d - 1]) for d in range(1, NZ)]
    out[ob, cols] = bcol[...]
    for m in a2:
        m.wait_recv()
    last = []
    whole = lambda q: out.at[rows_of(mine + q * pa, pa)]
    parts = ring_gather(copy, out, mine, pa, x, right, left, wx, NX)
    got = next(parts)
    last.append(copy(whole(x), whole(x), other))
    last.append(copy(whole(got), whole(got), other))
    got = next(parts)
    last.append(copy(whole(got), whole(got), other))
    for m in b4:
        m.wait_recv()
    last.append(copy(out.at[ob], out.at[ob], other))
    got = next(parts)
    last.append(copy(whole(got), whole(got), other))
    for m in last:
        m.wait_recv()
    for m in made:
        m.wait_send()


def total_grid(v, scale):
    n, w = v.shape
    half = n // 2
    nb = 64
    pa = (half - nb) // NX
    scratch = [
        (half, w), (half, w), (8, pa // 2, w), (NZ - 1, nb, 128), (NX - 1, nb // NX, 128),
        (nb, 128), (nb, 128), (NZ - 1, pa, 128), (pa, 128),
    ]
    return communicate(functools.partial(total_kernel, scale), "total_grid", (n, w), [v], scratch, 2 + 7 + 6 + 3 + 7 + 3 + 7 + 7 + 6 + 5, 3)


def part_kernel(both, out, ch, cl, tmp):
    c, x, _, y = place()
    nq = ch.shape[0]
    ch[...], cl[...] = halves(both[pl.ds(0, nq)])
    for s in range(9):
        upper = s < 8 - x
        rb = jnp.where(upper, x, 7 - x)
        cb = jnp.where(upper, x + s, s - 1)
        r, q = lanes_of(rb * 128, 128), lanes_of(cb * 128, 128)
        prod = dot3((ch[:, r], cl[:, r]), (ch[:, q], cl[:, q]), TN)
        own = (lax.div(rb, 2) == y).astype(F32)
        tmp[...] = own * both[rows_of(nq + lax.rem(rb, 2) * 128, 128), q] - prod
        out[:, pl.ds(s * 128, 128)] = tmp[rows_of(c * 64, 64), :]


def gram_part(both, nq):
    space = pl.BlockSpec(memory_space=pltpu.VMEM)
    w = both.shape[1]
    return pl.pallas_call(
        part_kernel,
        name="gram_part",
        out_shape=jax.ShapeDtypeStruct((64, 9 * 128), F32),
        in_specs=[space],
        out_specs=space,
        scratch_shapes=[pltpu.VMEM((nq, w), BF16), pltpu.VMEM((nq, w), BF16), pltpu.VMEM((128, 128), F32)],
    )(both)


def finish_kernel(part, s_ref, p_ref, out, g, m_ref, yb, fin, mid, whole, th, tl, send, recv):
    c, x, z, y = place()
    wx, wy = (lambda q: lax.rem(q, NX)), (lambda q: lax.rem(q, NY))
    other = grid_id(z, x, 1 - c)
    xr, xl = grid_id(z, wx(x + 1), c), grid_id(z, wx(x + NX - 1), c)
    ys = [{"band": wy(y + d)} for d in range(1, NY)]
    right, left = ys[0], ys[2]
    before, after, far = wy(y + NY - 1), wy(y + 1), wy(y + 2)
    greet([other, xr, xl] + ys)
    made = []

    def plan(src, dst, device):
        at = len(made)
        made.append(
            pltpu.make_async_remote_copy(
                src_ref=src, dst_ref=dst, send_sem=send.at[at], recv_sem=recv.at[at],
                device_id=device, device_id_type=MESH,
            )
        )
        return made[-1]

    def copy(src, dst, device):
        p = plan(src, dst, device)
        p.start()
        return p

    n = p_ref.shape[0]
    h, w4 = n // 2, n // 4
    first = lambda q: rows_of(q * n, h)
    second = lambda q: rows_of(q * n + h, h)
    ng = part.shape[0]
    q = ng // NY
    r1 = [copy(part.at[rows_of(wy(y + d) * q, q)], yb.at[d - 1], ys[d - 1]) for d in (2, 1, 3)]
    a = [copy(s_ref.at[rows_of(far * n + i * w4, w4)], mid.at[0, pl.ds(i * w4, w4)], right) for i in range(1)]
    b = [copy(s_ref.at[rows_of(far * n + h + i * w4, w4)], mid.at[1, pl.ds(i * w4, w4)], left) for i in range(1)]
    for m in r1:
        m.wait_recv()
    t = part[rows_of(y * q, q)]
    for d in range(NY - 1):
        t = t + yb[d]
    fin[...] = t
    base = c * (ng * NX)
    at = rows_of(base + x * ng + y * q, q)
    r2 = [copy(fin, g.at[at], ys[d - 1]) for d in (2, 1, 3)]
    a += [copy(s_ref.at[rows_of(far * n + i * w4, w4)], mid.at[0, pl.ds(i * w4, w4)], right) for i in range(1, 2)]
    b += [copy(s_ref.at[rows_of(far * n + h + i * w4, w4)], mid.at[1, pl.ds(i * w4, w4)], left) for i in range(1, 2)]
    cc = copy(s_ref.at[second(after)], mid.at[2], right)
    dd = copy(s_ref.at[first(before)], mid.at[3], left)
    g[at] = t
    for m in r2:
        m.wait_recv()
    block = lambda b: g.at[rows_of(base + b * ng, ng)]
    last = []
    parts = ring_gather(copy, g, base, ng, x, xr, xl, wx, NX)
    got = next(parts)
    last.append(copy(block(x), block(x), other))
    last.append(copy(block(got), block(got), other))
    for got in parts:
        last.append(copy(block(got), block(got), other))
    for m in a:
        m.wait_recv()
    mid[6] = mid[0] + s_ref[first(after)]
    ee = copy(mid.at[6], mid.at[4], right)
    for m in b:
        m.wait_recv()
    mid[7] = mid[1] + s_ref[second(before)]
    ff = copy(mid.at[7], mid.at[5], left)
    for m in last:
        m.wait_recv()
    up = lambda b: whole.at[first(b)]
    down = lambda b: whole.at[second(b)]
    own = [
        plan(up(y), up(y), right), plan(down(y), down(y), left),
        plan(down(y), down(y), right), plan(up(y), up(y), left),
    ]
    pass_on = [plan(up(before), up(before), right), plan(down(after), down(after), left)]

    def scattered():
        for m in (cc, dd, ee):
            m.wait_recv()
        whole[first(y)] = p_ref[pl.ds(0, h)] - (s_ref[first(y)] + (mid[3] + mid[4]))
        own[0].start()
        ff.wait_recv()
        whole[second(y)] = p_ref[pl.ds(h, h)] - (s_ref[second(y)] + (mid[2] + mid[5]))
        for m in own[1:]:
            m.start()

    def passed():
        for i in range(2):
            own[i].wait_recv()
            pass_on[i].start()

    factorize(g, m_ref, th, tl, {SCATTERED_AT: scattered, PASSED_AT: passed})

    def product(b):
        return dot3(halves(m_ref[rows_of(y * n, n), lanes_of(b * n, n)]), halves(whole[rows_of(b * n, n), :]), NN)

    out[...] = product(y)
    own[2].wait_recv()
    out[...] = out[...] + product(before)
    own[3].wait_recv()
    out[...] = out[...] + product(after)
    for m in pass_on:
        m.wait_recv()
    out[...] = out[...] + product(far)
    for m in made:
        m.wait_send()


def finish(part, s, p):
    n, w = p.shape
    ng, wg = part.shape
    total = n * NY
    space = pl.BlockSpec(memory_space=pltpu.VMEM)
    shapes = [(2 * NX * ng, wg), (total, total), (NY - 1, ng // NY, wg), (ng // NY, wg), (8, n // 2, w), (total, w)]
    return pl.pallas_call(
        finish_kernel,
        name="finish",
        out_shape=jax.ShapeDtypeStruct((n, w), F32),
        in_specs=[space] * 3,
        out_specs=space,
        scratch_shapes=[pltpu.VMEM(s_, F32) for s_ in shapes]
        + [pltpu.VMEM((B, total), BF16)] * 2
        + [pltpu.SemaphoreType.DMA((30,)), pltpu.SemaphoreType.DMA((30,))],
        compiler_params=pltpu.CompilerParams(collective_id=5, has_side_effects=True, vmem_limit_bytes=56 * 2**20),
    )(part, s, p)


def tdot(left, right):
    return lax.dot_general(left, right, (NT, ((), ())), precision=lax.Precision.HIGH, preferred_element_type=F32)


def ndot(left, right):
    return jnp.dot(left, right, precision=lax.Precision.HIGH)


def body(basis, panel):
    n_grid = panel.shape[1] * lax.axis_size("grid")
    rows_q = basis.shape[0]
    whole = gather_band(panel)
    both = total_grid(tdot(jnp.concatenate([basis, panel], 0), whole), 1.0 / n_grid)
    coeffs = both[:rows_q]
    outer = ndot(coeffs.T, basis)
    new_panel = finish(gram_part(both, rows_q), outer, panel)
    return (new_panel, coeffs)


def solution(mesh):
    placed = (P("band", "grid"), P("band", "grid"))
    return jax.shard_map(
        body, mesh=mesh, in_specs=placed, out_specs=(P("band", "grid"), P("band", None)), check_vma=False,
    )
```

```python
import functools

import jax
import jax.numpy as jnp
from jax import lax
from jax.experimental import pallas as pl
from jax.experimental.pallas import tpu as pltpu
from jax.sharding import PartitionSpec as P

F32, BF16 = jnp.float32, jnp.bfloat16

def halves(x):
    hi = x.astype(BF16)
    return hi, (x - hi.astype(F32)).astype(BF16)

def dot3(a, b, dims):
    (ah, al), (bh, bl) = a, b
    dg = lambda u, v: lax.dot_general(u, v, (dims, ((), ())), preferred_element_type=F32)
    return dg(ah, bh) + (dg(ah, bl) + dg(al, bh))

NN, TN, NT = ((1,), (0,)), ((0,), (0,)), ((1,), (1,))
BASE = 32

def base_block(w, at):
    n = w.shape[0]
    rows = w[at:at + BASE]
    lane = lax.broadcasted_iota(jnp.int32, (BASE, n), 1)
    sub = lax.broadcasted_iota(jnp.int32, (BASE, n), 0)
    cols = []
    for j in range(BASE):
        lo = j // 8 * 8
        cols.append(jnp.broadcast_to(rows[lo:, at + j:at + j + 1], (BASE - lo, n)))
    inside = (lane >= at) & (lane < at + BASE)
    v = jnp.where(inside, (lane == sub + at).astype(F32), rows)
    v = [v[8 * s:8 * s + 8] for s in range(BASE // 8)]
    cols = [[c[8 * s:8 * s + 8] for s in range(c.shape[0] // 8)] for c in cols]
    nb = BASE // 8
    sub8 = lax.broadcasted_iota(jnp.int32, (8, n), 0)
    bc = lambda x, i: jnp.broadcast_to(x[i:i + 1], (8, n))
    for j in range(BASE):
        s0, r0 = j // 8, j % 8
        c = cols[j]
        inv = lax.rsqrt(bc(c[0], r0))
        l = [x * inv for x in c]
        for jj in range(j + 1, BASE):
            s1, r1 = jj // 8, jj % 8
            f = bc(l[s1 - s0], r1)
            for s in range(s1, nb):
                cols[jj][s - s1] = cols[jj][s - s1] - l[s - s0] * f
        piv = bc(v[s0], r0) * inv
        l0 = jnp.where(sub8 > r0, l[0], 0.0)
        v[s0] = jnp.where(sub8 == r0, piv, v[s0] - l0 * piv)
        for s in range(s0 + 1, nb):
            v[s] = v[s] - l[s - s0] * piv
    return jnp.concatenate(v, 0)

def factor128(w):
    n = w.shape[0]
    lane = lax.broadcasted_iota(jnp.int32, (n, n), 1)
    row = lax.broadcasted_iota(jnp.int32, (n, n), 0)
    for at in range(0, n, BASE):
        v = base_block(w, at)
        end = at + BASE
        if end < n:
            parts = halves(v)
            upd = lax.dot_general(v, v, (TN, ((), ())), precision=lax.Precision.HIGHEST, preferred_element_type=F32)
            below = w[end:]
            l2 = lane[end:]
            below = jnp.where((l2 >= at) & (l2 < end), 0.0, below) - upd[end:]
            w = jnp.concatenate(([w[:at]] if at else []) + [v, below], 0)
        else:
            w = jnp.concatenate([w[:at], v], 0)
    return jnp.where(lane <= row, w, 0.0)

B = 128


SCATTERED_AT, PASSED_AT = 0, 3


def factorize(g_ref, m_ref, th, tl, between):
    n = m_ref.shape[0]
    nb = n // B
    hb = g_ref.shape[0] // 2
    for t in range(nb // 2):
        for c in range(2):
            src = pl.ds(c * hb + t * 64, 64)
            m_ref[pl.ds(t * B + c * 64, 64), pl.ds(t * B, n - t * B)] = g_ref[src, pl.ds(0, n - t * B)]
            u = nb - 1 - t
            m_ref[pl.ds(u * B + c * 64, 64), pl.ds(u * B, n - u * B)] = g_ref[src, pl.ds(n - t * B, n - u * B)]

    def step(k, _):
        r = pl.multiple_of(k * B, B)
        inv = factor128(m_ref[pl.ds(r, B), pl.ds(r, B)])
        t = dot3(halves(inv), halves(m_ref[pl.ds(r, B), :]), NN)
        m_ref[pl.ds(r, B), :] = t
        m_ref[pl.ds(r, B), pl.ds(r, B)] = inv
        hi, lo = halves(m_ref[pl.ds(r, B), :])
        th[...] = hi
        tl[...] = lo

        def rest(i, _):
            q = pl.multiple_of(i * B, B)
            m_ref[pl.ds(q, B), pl.ds(r, B)] = jnp.zeros((B, B), F32)
            f = (th[:, pl.ds(q, B)], tl[:, pl.ds(q, B)])
            m_ref[pl.ds(q, B), :] = m_ref[pl.ds(q, B), :] - dot3(f, (th[...], tl[...]), TN)
            return 0
        lax.fori_loop(k + 1, nb, rest, 0)
        for when, act in between.items():
            pl.when(k == when)(act)
        return 0
    lax.fori_loop(0, nb, step, 0)
    for t in range(nb - 1):
        m_ref[pl.ds(t * B, B), pl.ds(t * B + B, n - t * B - B)] = jnp.zeros((B, n - t * B - B), F32)


MESH = pl.DeviceIdType.MESH
NX, NZ, NY = 4, 8, 4


def place():
    g = lax.axis_index("grid")
    return lax.rem(g, 2), lax.rem(lax.div(g, 2), NX), lax.div(g, 2 * NX), lax.axis_index("band")


def grid_id(z, x, c):
    return {"grid": (z * NX + x) * 2 + c}


def sender(send, recv):
    made = []

    def plan(src, dst, device):
        at = len(made)
        made.append(
            pltpu.make_async_remote_copy(
                src_ref=src, dst_ref=dst, send_sem=send.at[at], recv_sem=recv.at[at],
                device_id=device, device_id_type=MESH,
            )
        )
        return made[-1]

    def copy(src, dst, device):
        started = plan(src, dst, device)
        started.start()
        return started

    return plan, copy, made


def greet(devices):
    barrier = pltpu.get_barrier_semaphore()
    for device in devices:
        pl.semaphore_signal(barrier, inc=1, device_id=device, device_id_type=MESH)
    pl.semaphore_wait(barrier, len(devices))


def rows_of(start, count):
    return pl.ds(pl.multiple_of(start, 8), count)


def lanes_of(start, count):
    return pl.ds(pl.multiple_of(start, 128), count)


def ring_gather(copy, out, base, count, mine, right, left, wrap, size):
    half = count // 2
    first = lambda q: out.at[rows_of(base + q * count, half)]
    second = lambda q: out.at[rows_of(base + q * count + half, half)]
    a = copy(first(mine), first(mine), right)
    b = copy(second(mine), second(mine), left)
    c = copy(second(mine), second(mine), right)
    d = copy(first(mine), first(mine), left)
    before, after, far = wrap(mine + size - 1), wrap(mine + 1), wrap(mine + 2)
    a.wait_recv()
    e = copy(first(before), first(before), right)
    b.wait_recv()
    f = copy(second(after), second(after), left)
    c.wait_recv()
    yield before
    d.wait_recv()
    yield after
    e.wait_recv()
    f.wait_recv()
    yield far


def step_kernel(
    scale, q_ref, p_ref, out, coeffs, wh, wl, ch, cl, th, tl, pg, v, pair, acc, ring, zb, zfin, fin,
    pp, ct, rs, part, s_ref, g, m_ref, yb, gfin, mid, whole, send, recv,
):
    c, x, z, y = place()
    nq, npan = q_ref.shape[0], p_ref.shape[0]
    half = v.shape[1] // 2
    pa = half // NX
    h = pa // 2
    zrow = pa // (NZ // 2)
    wx, wz, wy = (lambda q: lax.rem(q, NX)), (lambda q: lax.rem(q, NZ)), (lambda q: lax.rem(q, NY))
    other = grid_id(z, x, 1 - c)
    right, left = grid_id(z, wx(x + 1), c), grid_id(z, wx(x + NX - 1), c)
    zs = [grid_id(wz(z + d), x, c) for d in range(1, NZ)]
    north, south = {"band": wy(y + 1)}, {"band": wy(y + NY - 1)}
    ys = [{"band": lax.rem(y + d, NY)} for d in range(1, NY)]
    greet([other, right, left] + ys + zs)
    plan, copy, made = sender(send, recv)
    mine, theirs = c * half, (1 - c) * half
    xb, xa, xf = wx(x + NX - 1), wx(x + 1), wx(x + 2)
    yb_, ya, yf = wy(y + NY - 1), wy(y + 1), wy(y + 2)
    hp = npan // 2
    p1, p2 = p_ref.at[pl.ds(0, hp)], p_ref.at[pl.ds(hp, hp)]
    gs = [copy(p1, pg.at[0], north), copy(p2, pg.at[1], south), copy(p2, pg.at[2], north), copy(p1, pg.at[3], south)]
    at = [
        (y * npan, y * npan + hp), (yb_ * npan, ya * npan + hp),
        (yb_ * npan + hp, ya * npan), (yf * npan, yf * npan + hp),
    ]
    wh[pl.ds(0, nq)], wl[pl.ds(0, nq)] = halves(q_ref[...])
    wh[pl.ds(nq, npan)], wl[pl.ds(nq, npan)] = halves(p_ref[...])
    n = wh.shape[0]
    tile = 256

    def product(s, rows):
        ph, plo = halves(rows)

        def some(i, _):
            r = rows_of(i * tile, tile)
            v[s, r, :] = dot3((wh[r, :], wl[r, :]), (ph, plo), NT)
            return 0

        lax.fori_loop(0, n // tile, some, 0)

    st = [dict() for _ in range(4)]
    piece = lambda q: rows_of(q * pa, pa)
    up = lambda q: rows_of(q * pa, h)
    down = lambda q: rows_of(q * pa + h, h)
    zpart = lambda q: (rows_of(x * pa + lax.div(q, 2) * zrow, zrow), lanes_of(lax.rem(q, 2) * 128, 128))

    def s0(s):
        if s == 0:
            product(0, p_ref[...])
        else:
            if s == 1:
                gs[0].wait_recv()
                gs.append(copy(pg.at[0], pg.at[4], north))
                gs[1].wait_recv()
                gs.append(copy(pg.at[1], pg.at[5], south))
            else:
                gs[2 * s - 2].wait_recv()
                gs[2 * s - 1].wait_recv()
            product(s, jnp.concatenate([pg[2 * s - 2], pg[2 * s - 1]], 0))
        st[s]["pair"] = copy(v.at[s, rows_of(theirs, half)], pair.at[s], other)

    def s1(s):
        st[s]["pair"].wait_recv()
        acc[s] = v[s, rows_of(mine, half), :] + pair[s]
        st[s]["m"] = [
            copy(acc.at[s, up(xf)], ring.at[s, 0], right), copy(acc.at[s, down(xf)], ring.at[s, 1], left),
            copy(acc.at[s, down(xa)], ring.at[s, 2], right), copy(acc.at[s, up(xb)], ring.at[s, 3], left),
        ]

    def s2(s):
        m = st[s]["m"]
        m[0].wait_recv()
        ring[s, 6] = acc[s, up(xa), :] + ring[s, 0]
        m.append(copy(ring.at[s, 6], ring.at[s, 4], right))
        m[1].wait_recv()
        ring[s, 7] = acc[s, down(xb), :] + ring[s, 1]
        m.append(copy(ring.at[s, 7], ring.at[s, 5], left))

    def s3(s):
        for m in st[s]["m"][2:]:
            m.wait_recv()
        acc[s, up(x), :] = acc[s, up(x), :] + (ring[s, 3] + ring[s, 4])
        acc[s, down(x), :] = acc[s, down(x), :] + (ring[s, 2] + ring[s, 5])
        st[s]["z"] = [copy(acc.at[(s,) + zpart(wz(z + d))], zb.at[s, d - 1], zs[d - 1]) for d in range(1, NZ)]

    def s4(s):
        for m in st[s]["z"]:
            m.wait_recv()
        r, l = zpart(z)
        t = acc[s, r, l]
        for d in range(NZ - 1):
            t = t + zb[s, d]
        t = t * scale
        zfin[s] = t
        r = rows_of(mine + x * pa + lax.div(z, 2) * zrow, zrow)
        st[s]["zz"] = [copy(zfin.at[s], fin.at[s, r, l], zs[d - 1]) for d in range(1, NZ)]
        fin[s, r, l] = t

    def s5(s):
        for m in st[s]["zz"]:
            m.wait_recv()
        f = lambda r: fin.at[s, r]
        fu = lambda q: f(rows_of(mine + q * pa, h))
        fd = lambda q: f(rows_of(mine + q * pa + h, h))
        st[s]["x"] = [
            copy(fu(x), fu(x), right), copy(fd(x), fd(x), left), copy(fd(x), fd(x), right), copy(fu(x), fu(x), left),
        ]
        whole = f(rows_of(mine + x * pa, pa))
        st[s]["o"] = [copy(whole, whole, other)]

    def s6(s):
        f = lambda r: fin.at[s, r]
        fu, fd = f(rows_of(mine + xb * pa, h)), f(rows_of(mine + xa * pa + h, h))
        m = st[s]["x"]
        m[0].wait_recv()
        m.append(copy(fu, fu, right))
        m[1].wait_recv()
        m.append(copy(fd, fd, left))

    def s7(s):
        m = st[s]["x"]
        m[2].wait_recv()
        m[3].wait_recv()
        for q in (xb, xa):
            whole = fin.at[s, rows_of(mine + q * pa, pa)]
            st[s]["o"].append(copy(whole, whole, other))
        m[4].wait_recv()
        m[5].wait_recv()
        whole = fin.at[s, rows_of(mine + xf * pa, pa)]
        st[s]["o"].append(copy(whole, whole, other))

    def s8(s):
        for m in st[s]["o"]:
            m.wait_recv()
        for i in range(2):
            to, frm = lanes_of(at[s][i], hp), pl.ds(i * hp, hp)
            block = fin[s, pl.ds(0, nq), frm]
            coeffs[:, to] = block
            ch[:, to], cl[:, to] = halves(block)
            pp[:, to] = fin[s, pl.ds(nq, npan), frm]

    rest = {}

    def s9(s):
        t = dot3(halves(fin[s, pl.ds(0, nq), :]), (wh[pl.ds(0, nq)], wl[pl.ds(0, nq)]), TN)
        s_ref[s] = t
        lo, hi = s_ref.at[s, pl.ds(0, hp)], s_ref.at[s, pl.ds(hp, hp)]
        if s == 1:
            rest["c"] = copy(hi, mid.at[2], north)
            rest["d"] = copy(lo, mid.at[3], south)
        if s == 3:
            rest["a"] = copy(lo, mid.at[0], north)
            rest["b"] = copy(hi, mid.at[1], south)

    ng = part.shape[0]
    gq = ng // NY

    def g0():
        for u, rb in enumerate((x, 7 - x)):
            ct[...] = coeffs[:, lanes_of(rb * 128, 128)].T
            rs[pl.ds(u * 64, 64), pl.ds(0, nq)] = ct[rows_of(c * 64, 64), :]
        prod = dot3(halves(rs[:, pl.ds(0, nq)]), (ch[...], cl[...]), NN)
        rs[...] = prod
        for k in range(9):
            first = k < 8 - x
            rb = jnp.where(first, x, 7 - x)
            cb = jnp.where(first, x + k, k - 1)
            u = jnp.where(first, 0, 1)
            l = lanes_of(cb * 128, 128)
            own = (lax.div(rb, 2) == y).astype(F32)
            part[:, pl.ds(k * 128, 128)] = own * pp[rows_of(lax.rem(rb, 2) * 128 + c * 64, 64), l] - rs[rows_of(u * 64, 64), l]
        rest["r1"] = [copy(part.at[rows_of(wy(y + d) * gq, gq)], yb.at[d - 1], ys[d - 1]) for d in (2, 1, 3)]

    gbase = c * (ng * NX)

    def g1():
        for m in rest["r1"]:
            m.wait_recv()
        t = part[rows_of(y * gq, gq)]
        for d in range(NY - 1):
            t = t + yb[d]
        gfin[...] = t
        to = rows_of(gbase + x * ng + y * gq, gq)
        rest["r2"] = [copy(gfin, g.at[to], ys[d - 1]) for d in (2, 1, 3)]
        g[to] = t

    def g2():
        for m in rest["r2"]:
            m.wait_recv()
        block = lambda b: g.at[rows_of(gbase + b * ng, ng)]
        last = []
        parts = ring_gather(copy, g, gbase, ng, x, right, left, wx, NX)
        got = next(parts)
        last.append(copy(block(x), block(x), other))
        last.append(copy(block(got), block(got), other))
        for got in parts:
            last.append(copy(block(got), block(got), other))
        rest["last"] = last

    def g3():
        rest["a"].wait_recv()
        mid[6] = mid[0] + s_ref[2, pl.ds(hp, hp), :]
        rest["e"] = copy(mid.at[6], mid.at[4], north)
        rest["b"].wait_recv()
        mid[7] = mid[1] + s_ref[2, pl.ds(0, hp), :]
        rest["f"] = copy(mid.at[7], mid.at[5], south)
        for m in rest["last"]:
            m.wait_recv()

    stages = (s0, s1, s2, s3, s4, s5, s6, s7, s8, s9)
    order = [(START[s] + AFTER[k], s, stages[k]) for s in range(4) for k in range(9)]
    order += [(START[s] + AFTER[8] + 0.1, s, s9) for s in range(3)]
    for _, s, stage in sorted(order, key=lambda e: e[:2]):
        stage(s)
    g0()
    s9(3)
    g1()
    g2()
    g3()
    first = lambda b: rows_of(b * npan, hp)
    second = lambda b: rows_of(b * npan + hp, hp)
    upper = lambda b: whole.at[first(b)]
    lower = lambda b: whole.at[second(b)]
    own = [
        plan(upper(y), upper(y), north), plan(lower(y), lower(y), south),
        plan(lower(y), lower(y), north), plan(upper(y), upper(y), south),
    ]
    pass_on = [plan(upper(yb_), upper(yb_), north), plan(lower(ya), lower(ya), south)]

    def scattered():
        rest["d"].wait_recv()
        rest["e"].wait_recv()
        whole[first(y)] = p_ref[pl.ds(0, hp)] - (s_ref[0, pl.ds(0, hp), :] + (mid[3] + mid[4]))
        own[0].start()
        rest["c"].wait_recv()
        rest["f"].wait_recv()
        whole[second(y)] = p_ref[pl.ds(hp, hp)] - (s_ref[0, pl.ds(hp, hp), :] + (mid[2] + mid[5]))
        for m in own[1:]:
            m.start()

    def passed():
        for i in range(2):
            own[i].wait_recv()
            pass_on[i].start()

    factorize(g, m_ref, th, tl, {SCATTERED_AT: scattered, PASSED_AT: passed})

    def share(b):
        return dot3(halves(m_ref[rows_of(y * npan, npan), lanes_of(b * npan, npan)]), halves(whole[rows_of(b * npan, npan), :]), NN)

    out[...] = share(y)
    own[2].wait_recv()
    out[...] = out[...] + share(yb_)
    own[3].wait_recv()
    out[...] = out[...] + share(ya)
    for m in pass_on:
        m.wait_recv()
    out[...] = out[...] + share(yf)
    for m in made:
        m.wait_send()


START = (3.0, 13.0, 24.5, 36.0)
AFTER = (0.0, 2.0, 5.0, 8.0, 15.0, 22.0, 25.0, 28.0, 30.0)


def step(basis, panel, scale):
    nq, w = basis.shape
    npan = panel.shape[0]
    total = npan * NY
    n = nq + npan
    half = n // 2
    pa = half // NX
    hp = npan // 2
    space = pl.BlockSpec(memory_space=pltpu.VMEM)
    short = [(n, w), (n, w), (nq, total), (nq, total), (B, total), (B, total)]
    shapes = [
        (6, hp, w), (4, n, 2 * hp), (4, half, 2 * hp), (4, half, 2 * hp), (4, 8, pa // 2, 2 * hp),
        (4, NZ - 1, pa * 2 // NZ, 128), (4, pa * 2 // NZ, 128), (4, n, 2 * hp),
        (npan, total), (128, nq), (128, total), (64, 9 * 128), (4, npan, w), (512, 9 * 128), (total, total),
        (NY - 1, 64 // NY, 9 * 128), (64 // NY, 9 * 128), (8, hp, w), (total, w),
    ]
    copies = 6 + 4 * (1 + 6 + 7 + 7 + 6 + 4) + 28
    return pl.pallas_call(
        functools.partial(step_kernel, scale),
        name="step",
        out_shape=[jax.ShapeDtypeStruct((npan, w), F32), jax.ShapeDtypeStruct((nq, total), F32)],
        in_specs=[space] * 2,
        out_specs=[space] * 2,
        scratch_shapes=[pltpu.VMEM(s_, BF16) for s_ in short] + [pltpu.VMEM(s_, F32) for s_ in shapes]
        + [pltpu.SemaphoreType.DMA((copies,)), pltpu.SemaphoreType.DMA((copies,))],
        compiler_params=pltpu.CompilerParams(collective_id=1, has_side_effects=True, vmem_limit_bytes=60 * 2**20),
    )(basis, panel)


def body(basis, panel):
    n_grid = panel.shape[1] * lax.axis_size("grid")
    return tuple(step(basis, panel, 1.0 / n_grid))


def solution(mesh):
    placed = (P("band", "grid"), P("band", "grid"))
    return jax.shard_map(
        body, mesh=mesh, in_specs=placed, out_specs=(P("band", "grid"), P("band", None)), check_vma=False,
    )
```

```python
import functools

import jax
import jax.numpy as jnp
from jax import lax
from jax.experimental import pallas as pl
from jax.experimental.pallas import tpu as pltpu
from jax.sharding import PartitionSpec as P

F32, BF16 = jnp.float32, jnp.bfloat16

def halves(x):
    hi = x.astype(BF16)
    return hi, (x - hi.astype(F32)).astype(BF16)

def dot3(a, b, dims):
    (ah, al), (bh, bl) = a, b
    dg = lambda u, v: lax.dot_general(u, v, (dims, ((), ())), preferred_element_type=F32)
    return dg(ah, bh) + (dg(ah, bl) + dg(al, bh))

NN, TN, NT = ((1,), (0,)), ((0,), (0,)), ((1,), (1,))
BASE = 32

def base_block(w, at):
    n = w.shape[0]
    rows = w[at:at + BASE]
    lane = lax.broadcasted_iota(jnp.int32, (BASE, n), 1)
    sub = lax.broadcasted_iota(jnp.int32, (BASE, n), 0)
    cols = []
    for j in range(BASE):
        lo = j // 8 * 8
        cols.append(jnp.broadcast_to(rows[lo:, at + j:at + j + 1], (BASE - lo, n)))
    inside = (lane >= at) & (lane < at + BASE)
    v = jnp.where(inside, (lane == sub + at).astype(F32), rows)
    v = [v[8 * s:8 * s + 8] for s in range(BASE // 8)]
    cols = [[c[8 * s:8 * s + 8] for s in range(c.shape[0] // 8)] for c in cols]
    nb = BASE // 8
    sub8 = lax.broadcasted_iota(jnp.int32, (8, n), 0)
    bc = lambda x, i: jnp.broadcast_to(x[i:i + 1], (8, n))
    for j in range(BASE):
        s0, r0 = j // 8, j % 8
        c = cols[j]
        inv = lax.rsqrt(bc(c[0], r0))
        l = [x * inv for x in c]
        for jj in range(j + 1, BASE):
            s1, r1 = jj // 8, jj % 8
            f = bc(l[s1 - s0], r1)
            for s in range(s1, nb):
                cols[jj][s - s1] = cols[jj][s - s1] - l[s - s0] * f
        piv = bc(v[s0], r0) * inv
        l0 = jnp.where(sub8 > r0, l[0], 0.0)
        v[s0] = jnp.where(sub8 == r0, piv, v[s0] - l0 * piv)
        for s in range(s0 + 1, nb):
            v[s] = v[s] - l[s - s0] * piv
    return jnp.concatenate(v, 0)

def factor128(w):
    n = w.shape[0]
    lane = lax.broadcasted_iota(jnp.int32, (n, n), 1)
    row = lax.broadcasted_iota(jnp.int32, (n, n), 0)
    for at in range(0, n, BASE):
        v = base_block(w, at)
        end = at + BASE
        if end < n:
            parts = halves(v)
            upd = dot3(parts, parts, TN)
            below = w[end:]
            l2 = lane[end:]
            below = jnp.where((l2 >= at) & (l2 < end), 0.0, below) - upd[end:]
            w = jnp.concatenate(([w[:at]] if at else []) + [v, below], 0)
        else:
            w = jnp.concatenate([w[:at], v], 0)
    return jnp.where(lane <= row, w, 0.0)

B = 128


SEGMENTS = ((0, 1, 0), (1, 4, 6), (4, 8, 3))
SPARE = 4


def factorize(g_ref, m_ref, th, tl, between):
    n = m_ref.shape[1]
    nb = n // B
    hb = g_ref.shape[0] // 2
    for t in range(nb // 2):
        for c in range(2):
            src = pl.ds(c * hb + t * 64, 64)
            m_ref[pl.ds(t * B + c * 64, 64), pl.ds(t * B, n - t * B)] = g_ref[src, pl.ds(0, n - t * B)]
            u = nb - 1 - t
            m_ref[pl.ds(u * B + c * 64, 64), pl.ds(u * B, n - u * B)] = g_ref[src, pl.ds(n - t * B, n - u * B)]
    th[:, pl.ds(n, SPARE * B)] = jnp.zeros((B, SPARE * B), BF16)
    tl[:, pl.ds(n, SPARE * B)] = jnp.zeros((B, SPARE * B), BF16)
    block = lambda i, count=1: pl.ds(pl.multiple_of(i * B, B), count * B)

    def update(i, count, k):
        q = block(i, count)
        m_ref[q, block(k)] = jnp.zeros((count * B, B), F32)
        m_ref[q, :] = m_ref[q, :] - dot3((th[:, q], tl[:, q]), (th[:, :n], tl[:, :n]), TN)

    def step(acts, count, k, _):
        inv = factor128(m_ref[block(k), block(k)])
        if count:
            update(k + 1, count, k - 1)
        t = dot3(halves(inv), halves(m_ref[block(k), :]), NN)
        m_ref[block(k), :] = t
        m_ref[block(k), block(k)] = inv
        hi, lo = halves(m_ref[block(k), :])
        th[:, :n] = hi
        tl[:, :n] = lo
        update(k + 1, 1, k)
        for when, act in acts.items():
            pl.when(k == when)(act)
        return 0

    for a, z, count in SEGMENTS:
        acts = {k: act for k, act in between.items() if a <= k < z}
        lax.fori_loop(a, z, functools.partial(step, acts, count), 0)


MESH = pl.DeviceIdType.MESH
NX, NZ, NY = 4, 8, 4


def place():
    g = lax.axis_index("grid")
    return lax.rem(g, 2), lax.rem(lax.div(g, 2), NX), lax.div(g, 2 * NX), lax.axis_index("band")


def grid_id(z, x, c):
    return {"grid": (z * NX + x) * 2 + c}


def sender(send, recv):
    made = []

    def plan(src, dst, device):
        at = len(made)
        made.append(
            pltpu.make_async_remote_copy(
                src_ref=src, dst_ref=dst, send_sem=send.at[at], recv_sem=recv.at[at],
                device_id=device, device_id_type=MESH,
            )
        )
        return made[-1]

    def copy(src, dst, device):
        started = plan(src, dst, device)
        started.start()
        return started

    return plan, copy, made


def greet(devices):
    barrier = pltpu.get_barrier_semaphore()
    for device in devices:
        pl.semaphore_signal(barrier, inc=1, device_id=device, device_id_type=MESH)
    pl.semaphore_wait(barrier, len(devices))


def rows_of(start, count):
    return pl.ds(pl.multiple_of(start, 8), count)


def lanes_of(start, count):
    return pl.ds(pl.multiple_of(start, 128), count)


def step_kernel(
    scale, q_ref, p_ref, out, coeffs, wh, wl, ch, cl, th, tl, rh, rl, pg, v, pair, acc, ring, zb, zfin, fin,
    pp, ct, rs, part, s_ref, g, m_ref, yb, gfin, mid, whole, send, recv,
):
    c, x, z, y = place()
    nq, npan = q_ref.shape[0], p_ref.shape[0]
    half = v.shape[1] // 2
    pa = half // NX
    h = pa // 2
    zrow = pa // (NZ // 2)
    wx, wz, wy = (lambda q: lax.rem(q, NX)), (lambda q: lax.rem(q, NZ)), (lambda q: lax.rem(q, NY))
    other = grid_id(z, x, 1 - c)
    right, left = grid_id(z, wx(x + 1), c), grid_id(z, wx(x + NX - 1), c)
    zs = [grid_id(wz(z + d), x, c) for d in range(1, NZ)]
    north, south = {"band": wy(y + 1)}, {"band": wy(y + NY - 1)}
    ys = [{"band": lax.rem(y + d, NY)} for d in range(1, NY)]
    greet([other, right, left] + ys + zs)
    plan, copy, made = sender(send, recv)
    mine, theirs = c * half, (1 - c) * half
    xb, xa, xf = wx(x + NX - 1), wx(x + 1), wx(x + 2)
    yb_, ya, yf = wy(y + NY - 1), wy(y + 1), wy(y + 2)
    hp = npan // 2
    p1, p2 = p_ref.at[pl.ds(0, hp)], p_ref.at[pl.ds(hp, hp)]
    gs = [copy(p1, pg.at[0], north), copy(p2, pg.at[1], south), copy(p2, pg.at[2], north), copy(p1, pg.at[3], south)]
    at = [
        (y * npan, y * npan + hp), (yb_ * npan, ya * npan + hp),
        (yb_ * npan + hp, ya * npan), (yf * npan, yf * npan + hp),
    ]
    wh[pl.ds(0, nq)], wl[pl.ds(0, nq)] = halves(q_ref[...])
    wh[pl.ds(nq, npan)], wl[pl.ds(nq, npan)] = halves(p_ref[...])
    n = wh.shape[0]
    tile = 256

    def product(s, rows):
        ph, plo = halves(rows)

        def some(i, _):
            r = rows_of(i * tile, tile)
            v[s, r, :] = dot3((wh[r, :], wl[r, :]), (ph, plo), NT)
            return 0

        lax.fori_loop(0, n // tile, some, 0)

    st = [dict() for _ in range(4)]
    piece = lambda q: rows_of(q * pa, pa)
    up = lambda q: rows_of(q * pa, h)
    down = lambda q: rows_of(q * pa + h, h)
    zpart = lambda q: (rows_of(x * pa + lax.div(q, 2) * zrow, zrow), lanes_of(lax.rem(q, 2) * 128, 128))

    def s0(s):
        if s == 0:
            product(0, p_ref[...])
        else:
            if s == 1:
                gs[0].wait_recv()
                gs.append(copy(pg.at[0], pg.at[4], north))
                gs[1].wait_recv()
                gs.append(copy(pg.at[1], pg.at[5], south))
            else:
                gs[2 * s - 2].wait_recv()
                gs[2 * s - 1].wait_recv()
            product(s, jnp.concatenate([pg[2 * s - 2], pg[2 * s - 1]], 0))
        st[s]["pair"] = copy(v.at[s, rows_of(theirs, half)], pair.at[s], other)

    def s1(s):
        st[s]["pair"].wait_recv()
        acc[s] = v[s, rows_of(mine, half), :] + pair[s]
        st[s]["m"] = [
            copy(acc.at[s, up(xf)], ring.at[s, 0], right), copy(acc.at[s, down(xf)], ring.at[s, 1], left),
            copy(acc.at[s, down(xa)], ring.at[s, 2], right), copy(acc.at[s, up(xb)], ring.at[s, 3], left),
        ]

    def s2(s):
        m = st[s]["m"]
        m[0].wait_recv()
        ring[s, 6] = acc[s, up(xa), :] + ring[s, 0]
        m.append(copy(ring.at[s, 6], ring.at[s, 4], right))
        m[1].wait_recv()
        ring[s, 7] = acc[s, down(xb), :] + ring[s, 1]
        m.append(copy(ring.at[s, 7], ring.at[s, 5], left))

    def s3(s):
        for m in st[s]["m"][2:]:
            m.wait_recv()
        acc[s, up(x), :] = acc[s, up(x), :] + (ring[s, 3] + ring[s, 4])
        acc[s, down(x), :] = acc[s, down(x), :] + (ring[s, 2] + ring[s, 5])
        st[s]["z"] = [copy(acc.at[(s,) + zpart(wz(z + d))], zb.at[s, d - 1], zs[d - 1]) for d in range(1, NZ)]

    def s4(s):
        for m in st[s]["z"]:
            m.wait_recv()
        r, l = zpart(z)
        t = acc[s, r, l]
        for d in range(NZ - 1):
            t = t + zb[s, d]
        t = t * scale
        zfin[s] = t
        r = rows_of(mine + x * pa + lax.div(z, 2) * zrow, zrow)
        st[s]["zz"] = [copy(zfin.at[s], fin.at[s, r, l], zs[d - 1]) for d in range(1, NZ)]
        fin[s, r, l] = t

    def s5(s):
        for m in st[s]["zz"]:
            m.wait_recv()
        f = lambda r: fin.at[s, r]
        fu = lambda q: f(rows_of(mine + q * pa, h))
        fd = lambda q: f(rows_of(mine + q * pa + h, h))
        st[s]["x"] = [
            copy(fu(x), fu(x), right), copy(fd(x), fd(x), left), copy(fd(x), fd(x), right), copy(fu(x), fu(x), left),
        ]
        whole = f(rows_of(mine + x * pa, pa))
        st[s]["o"] = [copy(whole, whole, other)]

    def s6(s):
        f = lambda r: fin.at[s, r]
        fu, fd = f(rows_of(mine + xb * pa, h)), f(rows_of(mine + xa * pa + h, h))
        m = st[s]["x"]
        m[0].wait_recv()
        m.append(copy(fu, fu, right))
        m[1].wait_recv()
        m.append(copy(fd, fd, left))

    def s7(s):
        m = st[s]["x"]
        m[2].wait_recv()
        m[3].wait_recv()
        for q in (xb, xa):
            whole = fin.at[s, rows_of(mine + q * pa, pa)]
            st[s]["o"].append(copy(whole, whole, other))
        m[4].wait_recv()
        m[5].wait_recv()
        whole = fin.at[s, rows_of(mine + xf * pa, pa)]
        st[s]["o"].append(copy(whole, whole, other))

    def s8(s):
        for m in st[s]["o"]:
            m.wait_recv()
        for i in range(2):
            to, frm = lanes_of(at[s][i], hp), pl.ds(i * hp, hp)
            block = fin[s, pl.ds(0, nq), frm]
            coeffs[:, to] = block
            ch[:, to], cl[:, to] = halves(block)
            pp[:, to] = fin[s, pl.ds(nq, npan), frm]

    rest = {}

    hq = hp // 2
    part_of = lambda i: pl.ds(i * hq, hq)

    def far_sum(i):
        rest["a", i] = copy(s_ref.at[3, part_of(i)], mid.at[0, part_of(i)], north)
        rest["b", i] = copy(s_ref.at[3, part_of(2 + i)], mid.at[1, part_of(i)], south)

    def near_sum(i):
        rest["a", i].wait_recv()
        mid[6, part_of(i)] = mid[0, part_of(i)] + s_ref[2, part_of(2 + i), :]
        rest["e", i] = copy(mid.at[6, part_of(i)], mid.at[4, part_of(i)], north)
        rest["b", i].wait_recv()
        mid[7, part_of(i)] = mid[1, part_of(i)] + s_ref[2, part_of(i), :]
        rest["f", i] = copy(mid.at[7, part_of(i)], mid.at[5, part_of(i)], south)

    def s9(s):
        t = dot3(halves(fin[s, pl.ds(0, nq), :]), (wh[pl.ds(0, nq)], wl[pl.ds(0, nq)]), TN)
        s_ref[s] = t
        lo, hi = s_ref.at[s, pl.ds(0, hp)], s_ref.at[s, pl.ds(hp, hp)]
        if s == 1:
            rest["c"] = copy(hi, mid.at[2], north)
            rest["d"] = copy(lo, mid.at[3], south)
        if s == 3:
            far_sum(0)

    ng = part.shape[0]
    gq = ng // NY

    def g0():
        for u, rb in enumerate((x, 7 - x)):
            ct[...] = coeffs[:, lanes_of(rb * 128, 128)].T
            rs[pl.ds(u * 64, 64), pl.ds(0, nq)] = ct[rows_of(c * 64, 64), :]
        prod = dot3(halves(rs[:, pl.ds(0, nq)]), (ch[...], cl[...]), NN)
        rs[...] = prod
        for k in range(9):
            first = k < 8 - x
            rb = jnp.where(first, x, 7 - x)
            cb = jnp.where(first, x + k, k - 1)
            u = jnp.where(first, 0, 1)
            l = lanes_of(cb * 128, 128)
            own = (lax.div(rb, 2) == y).astype(F32)
            part[:, pl.ds(k * 128, 128)] = own * pp[rows_of(lax.rem(rb, 2) * 128 + c * 64, 64), l] - rs[rows_of(u * 64, 64), l]
        rest["r1"] = [copy(part.at[rows_of(wy(y + d) * gq, gq)], yb.at[d - 1], ys[d - 1]) for d in (2, 1, 3)]

    gbase = c * (ng * NX)

    def g1():
        for m in rest["r1"]:
            m.wait_recv()
        t = part[rows_of(y * gq, gq)]
        for d in range(NY - 1):
            t = t + yb[d]
        gfin[...] = t
        to = rows_of(gbase + x * ng + y * gq, gq)
        rest["r2"] = [copy(gfin, g.at[to], ys[d - 1]) for d in (2, 1, 3)]
        far_sum(1)
        g[to] = t

    def g2():
        for m in rest["r2"]:
            m.wait_recv()
        hg = ng // 2
        upper = lambda b: g.at[rows_of(gbase + b * ng, hg)]
        lower = lambda b: g.at[rows_of(gbase + b * ng + hg, hg)]
        whole_of = lambda b: g.at[rows_of(gbase + b * ng, ng)]
        m = [
            copy(upper(x), upper(x), right), copy(lower(x), lower(x), left),
            copy(lower(x), lower(x), right), copy(upper(x), upper(x), left),
        ]
        last = [copy(whole_of(x), whole_of(x), other)]
        near_sum(0)
        m[0].wait_recv()
        m.append(copy(upper(xb), upper(xb), right))
        m[1].wait_recv()
        m.append(copy(lower(xa), lower(xa), left))
        m[2].wait_recv()
        last.append(copy(whole_of(xb), whole_of(xb), other))
        m[3].wait_recv()
        last.append(copy(whole_of(xa), whole_of(xa), other))
        near_sum(1)
        m[4].wait_recv()
        m[5].wait_recv()
        last.append(copy(whole_of(xf), whole_of(xf), other))
        for q in last:
            q.wait_recv()

    stages = (s0, s1, s2, s3, s4, s5, s6, s7, s8, s9)
    order = [(START[s] + AFTER[k], s, stages[k]) for s in range(4) for k in range(9)]
    order += [(START[s] + AFTER[8] + 0.1, s, s9) for s in range(3)]
    for _, s, stage in sorted(order, key=lambda e: e[:2]):
        stage(s)
    g0()
    s9(3)
    g1()
    g2()
    upper = lambda b, at=0, count=hp: whole.at[rows_of(b * npan + at, count)]
    lower = lambda b, at=0, count=hp: whole.at[rows_of(b * npan + hp + at, count)]
    same = lambda ref, to: plan(ref, ref, to)
    early = [[same(upper(y, i * hq, hq), north), same(lower(y, i * hq, hq), south)] for i in range(2)]
    later = [same(lower(y), north), same(upper(y), south)]
    pass_on = [same(upper(yb_), north), same(lower(ya), south)]

    def split(b):
        r = rows_of(b * npan, npan)
        rh[r, :], rl[r, :] = halves(whole[r, :])

    def summed(i):
        def act():
            if i == 0:
                rest["d"].wait_recv()
                rest["c"].wait_recv()
            p = part_of(i)
            q = part_of(2 + i)
            rest["e", i].wait_recv()
            whole[rows_of(y * npan + i * hq, hq)] = p_ref[p] - (s_ref[0, p, :] + (mid[3, p] + mid[4, p]))
            early[i][0].start()
            rest["f", i].wait_recv()
            whole[rows_of(y * npan + hp + i * hq, hq)] = p_ref[q] - (s_ref[0, q, :] + (mid[2, p] + mid[5, p]))
            early[i][1].start()
            if i == 1:
                for m in later:
                    m.start()
        return act

    def passed():
        for i in range(2):
            early[0][i].wait_recv()
            early[1][i].wait_recv()
            pass_on[i].start()

    def near():
        split(y)
        for m in later:
            m.wait_recv()
        split(yb_)
        split(ya)

    factorize(g, m_ref, th, tl, dict(zip(HOOKS, (summed(0), summed(1), passed, near))))
    mine_rows = m_ref[rows_of(y * npan, npan), :]
    total = mine_rows.shape[1]
    row = lax.broadcasted_iota(jnp.int32, (npan, total), 0) + y * npan
    col = lax.broadcasted_iota(jnp.int32, (npan, total), 1)
    xh, xl = halves(jnp.where(col <= row, mine_rows, 0.0))
    ch[pl.ds(0, npan)], cl[pl.ds(0, npan)] = xh, xl
    for m in pass_on:
        m.wait_recv()
    split(yf)

    def columns(i, _):
        l = lanes_of(i * 256, 256)
        out[:, l] = dot3((ch[pl.ds(0, npan)], cl[pl.ds(0, npan)]), (rh[:, l], rl[:, l]), NN)
        return 0

    lax.fori_loop(0, out.shape[1] // 256, columns, 0)
    for m in made:
        m.wait_send()


HOOKS = (0, 1, 3, 6)
START = (3.0, 13.0, 24.5, 36.0)
AFTER = (0.0, 2.0, 5.0, 8.0, 15.0, 22.0, 25.0, 28.0, 30.0)


def step(basis, panel, scale):
    nq, w = basis.shape
    npan = panel.shape[0]
    total = npan * NY
    n = nq + npan
    half = n // 2
    pa = half // NX
    hp = npan // 2
    space = pl.BlockSpec(memory_space=pltpu.VMEM)
    short = [(n, w), (n, w), (nq, total), (nq, total)] + [(B, total + SPARE * B)] * 2 + [(total, w)] * 2
    shapes = [
        (6, hp, w), (4, n, 2 * hp), (4, half, 2 * hp), (4, half, 2 * hp), (4, 8, pa // 2, 2 * hp),
        (4, NZ - 1, pa * 2 // NZ, 128), (4, pa * 2 // NZ, 128), (4, n, 2 * hp),
        (npan, total), (128, nq), (128, total), (64, 9 * 128), (4, npan, w), (512, 9 * 128), (total + SPARE * B, total),
        (NY - 1, 64 // NY, 9 * 128), (64 // NY, 9 * 128), (8, hp, w), (total, w),
    ]
    copies = 6 + 4 * (1 + 6 + 7 + 7 + 6 + 4) + 34
    return pl.pallas_call(
        functools.partial(step_kernel, scale),
        name="step",
        out_shape=[jax.ShapeDtypeStruct((npan, w), F32), jax.ShapeDtypeStruct((nq, total), F32)],
        in_specs=[space] * 2,
        out_specs=[space] * 2,
        scratch_shapes=[pltpu.VMEM(s_, BF16) for s_ in short] + [pltpu.VMEM(s_, F32) for s_ in shapes]
        + [pltpu.SemaphoreType.DMA((copies,)), pltpu.SemaphoreType.DMA((copies,))],
        compiler_params=pltpu.CompilerParams(collective_id=1, has_side_effects=True, vmem_limit_bytes=60 * 2**20),
    )(basis, panel)


def body(basis, panel):
    n_grid = panel.shape[1] * lax.axis_size("grid")
    return tuple(step(basis, panel, 1.0 / n_grid))


def solution(mesh):
    placed = (P("band", "grid"), P("band", "grid"))
    return jax.shard_map(
        body, mesh=mesh, in_specs=placed, out_specs=(P("band", "grid"), P("band", None)), check_vma=False,
    )
```

```python
import functools

import jax
import jax.numpy as jnp
from jax import lax
from jax.experimental import pallas as pl
from jax.experimental.pallas import tpu as pltpu
from jax.sharding import PartitionSpec as P

F32, BF16 = jnp.float32, jnp.bfloat16

def halves(x):
    hi = x.astype(BF16)
    return hi, (x - hi.astype(F32)).astype(BF16)

def dot3(a, b, dims):
    (ah, al), (bh, bl) = a, b
    dg = lambda u, v: lax.dot_general(u, v, (dims, ((), ())), preferred_element_type=F32)
    return dg(ah, bh) + (dg(ah, bl) + dg(al, bh))

NN, TN, NT = ((1,), (0,)), ((0,), (0,)), ((1,), (1,))
BASE = 32

def base_block(w, at):
    n = w.shape[0]
    rows = w[at:at + BASE]
    lane = lax.broadcasted_iota(jnp.int32, (BASE, n), 1)
    sub = lax.broadcasted_iota(jnp.int32, (BASE, n), 0)
    cols = []
    for j in range(BASE):
        lo = j // 8 * 8
        cols.append(jnp.broadcast_to(rows[lo:, at + j:at + j + 1], (BASE - lo, n)))
    inside = (lane >= at) & (lane < at + BASE)
    v = jnp.where(inside, (lane == sub + at).astype(F32), rows)
    v = [v[8 * s:8 * s + 8] for s in range(BASE // 8)]
    cols = [[c[8 * s:8 * s + 8] for s in range(c.shape[0] // 8)] for c in cols]
    nb = BASE // 8
    sub8 = lax.broadcasted_iota(jnp.int32, (8, n), 0)
    bc = lambda x, i: jnp.broadcast_to(x[i:i + 1], (8, n))
    for j in range(BASE):
        s0, r0 = j // 8, j % 8
        c = cols[j]
        inv = lax.rsqrt(bc(c[0], r0))
        l = [x * inv for x in c]
        for jj in range(j + 1, BASE):
            s1, r1 = jj // 8, jj % 8
            f = bc(l[s1 - s0], r1)
            for s in range(s1, nb):
                cols[jj][s - s1] = cols[jj][s - s1] - l[s - s0] * f
        piv = bc(v[s0], r0) * inv
        l0 = jnp.where(sub8 > r0, l[0], 0.0)
        v[s0] = jnp.where(sub8 == r0, piv, v[s0] - l0 * piv)
        for s in range(s0 + 1, nb):
            v[s] = v[s] - l[s - s0] * piv
    return jnp.concatenate(v, 0)

def factor128(w):
    n = w.shape[0]
    lane = lax.broadcasted_iota(jnp.int32, (n, n), 1)
    row = lax.broadcasted_iota(jnp.int32, (n, n), 0)
    for at in range(0, n, BASE):
        v = base_block(w, at)
        end = at + BASE
        if end < n:
            parts = halves(v)
            upd = dot3(parts, parts, TN)
            below = w[end:]
            l2 = lane[end:]
            below = jnp.where((l2 >= at) & (l2 < end), 0.0, below) - upd[end:]
            w = jnp.concatenate(([w[:at]] if at else []) + [v, below], 0)
        else:
            w = jnp.concatenate([w[:at], v], 0)
    return jnp.where(lane <= row, w, 0.0)

B = 128


SEGMENTS = ((0, 1, 0), (1, 4, 6), (4, 8, 3))
SPARE = 4


def factorize(g_ref, m_ref, th, tl, between):
    n = m_ref.shape[1]
    nb = n // B
    hb = g_ref.shape[0] // 2
    for t in range(nb // 2):
        for c in range(2):
            src = pl.ds(c * hb + t * 64, 64)
            m_ref[pl.ds(t * B + c * 64, 64), pl.ds(t * B, n - t * B)] = g_ref[src, pl.ds(0, n - t * B)]
            u = nb - 1 - t
            m_ref[pl.ds(u * B + c * 64, 64), pl.ds(u * B, n - u * B)] = g_ref[src, pl.ds(n - t * B, n - u * B)]
    th[:, pl.ds(n, SPARE * B)] = jnp.zeros((B, SPARE * B), BF16)
    tl[:, pl.ds(n, SPARE * B)] = jnp.zeros((B, SPARE * B), BF16)
    block = lambda i, count=1: pl.ds(pl.multiple_of(i * B, B), count * B)

    def update(i, count, k):
        q = block(i, count)
        m_ref[q, block(k)] = jnp.zeros((count * B, B), F32)
        m_ref[q, :] = m_ref[q, :] - dot3((th[:, q], tl[:, q]), (th[:, :n], tl[:, :n]), TN)

    def step(acts, count, k, _):
        inv = factor128(m_ref[block(k), block(k)])
        if count:
            update(k + 1, count, k - 1)
        t = dot3(halves(inv), halves(m_ref[block(k), :]), NN)
        m_ref[block(k), :] = t
        m_ref[block(k), block(k)] = inv
        hi, lo = halves(m_ref[block(k), :])
        th[:, :n] = hi
        tl[:, :n] = lo
        update(k + 1, 1, k)
        for when, act in acts.items():
            pl.when(k == when)(act)
        return 0

    for a, z, count in SEGMENTS:
        acts = {k: act for k, act in between.items() if a <= k < z}
        lax.fori_loop(a, z, functools.partial(step, acts, count), 0)


MESH = pl.DeviceIdType.MESH
NX, NZ, NY = 4, 8, 4


def place():
    g = lax.axis_index("grid")
    return lax.rem(g, 2), lax.rem(lax.div(g, 2), NX), lax.div(g, 2 * NX), lax.axis_index("band")


def grid_id(z, x, c):
    return {"grid": (z * NX + x) * 2 + c}


def sender(send, recv):
    made = []

    def plan(src, dst, device):
        at = len(made)
        made.append(
            pltpu.make_async_remote_copy(
                src_ref=src, dst_ref=dst, send_sem=send.at[at], recv_sem=recv.at[at],
                device_id=device, device_id_type=MESH,
            )
        )
        return made[-1]

    def copy(src, dst, device):
        started = plan(src, dst, device)
        started.start()
        return started

    return plan, copy, made


def greet(devices):
    barrier = pltpu.get_barrier_semaphore()
    for device in devices:
        pl.semaphore_signal(barrier, inc=1, device_id=device, device_id_type=MESH)
    pl.semaphore_wait(barrier, len(devices))


def rows_of(start, count):
    return pl.ds(pl.multiple_of(start, 8), count)


def lanes_of(start, count):
    return pl.ds(pl.multiple_of(start, 128), count)


def step_kernel(
    scale, q_ref, p_ref, out, coeffs_hbm, wh, wl, ch, cl, th, tl, rh, rl, pg, v, pair, acc, ring, zb, zfin, fin,
    pp, ct, rs, part, s_ref, g, m_ref, yb, gfin, mid, whole, coeffs, send, recv, done,
):
    c, x, z, y = place()
    nq, npan = q_ref.shape[0], p_ref.shape[0]
    half = v.shape[1] // 2
    pa = half // NX
    h = pa // 2
    zrow = pa // (NZ // 2)
    wx, wz, wy = (lambda q: lax.rem(q, NX)), (lambda q: lax.rem(q, NZ)), (lambda q: lax.rem(q, NY))
    other = grid_id(z, x, 1 - c)
    right, left = grid_id(z, wx(x + 1), c), grid_id(z, wx(x + NX - 1), c)
    zs = [grid_id(wz(z + d), x, c) for d in range(1, NZ)]
    north, south = {"band": wy(y + 1)}, {"band": wy(y + NY - 1)}
    ys = [{"band": lax.rem(y + d, NY)} for d in range(1, NY)]
    greet([other, right, left] + ys + zs)
    plan, copy, made = sender(send, recv)
    mine, theirs = c * half, (1 - c) * half
    xb, xa, xf = wx(x + NX - 1), wx(x + 1), wx(x + 2)
    yb_, ya, yf = wy(y + NY - 1), wy(y + 1), wy(y + 2)
    hp = npan // 2
    p1, p2 = p_ref.at[pl.ds(0, hp)], p_ref.at[pl.ds(hp, hp)]
    lead, tail = pl.ds(0, hp // 4), pl.ds(hp // 4, hp - hp // 4)
    gs = [
        copy(p1, pg.at[0], north), copy(p2, pg.at[1], south),
        copy(p2.at[lead], pg.at[2, lead], north), copy(p1.at[lead], pg.at[3, lead], south),
    ]
    at = [
        (y * npan, y * npan + hp), (yb_ * npan, ya * npan + hp),
        (yf * npan, yf * npan + hp), (yb_ * npan + hp, ya * npan),
    ]
    wh[pl.ds(0, nq)], wl[pl.ds(0, nq)] = halves(q_ref[...])
    wh[pl.ds(nq, npan)], wl[pl.ds(nq, npan)] = halves(p_ref[...])
    n = wh.shape[0]
    tile = 256

    def product(s, rows):
        ph, plo = halves(rows)

        def some(i, _):
            r = rows_of(i * tile, tile)
            v[s, r, :] = dot3((wh[r, :], wl[r, :]), (ph, plo), NT)
            return 0

        lax.fori_loop(0, n // tile, some, 0)

    st = [dict() for _ in range(4)]
    piece = lambda q: rows_of(q * pa, pa)
    up = lambda q: rows_of(q * pa, h)
    down = lambda q: rows_of(q * pa + h, h)
    zpart = lambda q: (rows_of(x * pa + lax.div(q, 2) * zrow, zrow), lanes_of(lax.rem(q, 2) * 128, 128))

    def s0(s):
        if s == 0:
            product(0, p_ref[...])
        else:
            if s == 1:
                gs[0].wait_recv()
                gs.append(copy(pg.at[0], pg.at[4], north))
                gs.append(copy(p2.at[tail], pg.at[2, tail], north))
                gs[1].wait_recv()
                gs.append(copy(pg.at[1], pg.at[5], south))
                gs.append(copy(p1.at[tail], pg.at[3, tail], south))
            for m in {1: (), 2: (4, 6), 3: (2, 3, 5, 7)}[s]:
                gs[m].wait_recv()
            u = {1: 0, 2: 4, 3: 2}[s]
            product(s, jnp.concatenate([pg[u], pg[u + 1]], 0))
        st[s]["pair"] = copy(v.at[s, rows_of(theirs, half)], pair.at[s], other)

    def s1(s):
        st[s]["pair"].wait_recv()
        acc[s] = v[s, rows_of(mine, half), :] + pair[s]
        st[s]["m"] = [
            copy(acc.at[s, up(xf)], ring.at[s, 0], right), copy(acc.at[s, down(xf)], ring.at[s, 1], left),
            copy(acc.at[s, down(xa)], ring.at[s, 2], right), copy(acc.at[s, up(xb)], ring.at[s, 3], left),
        ]

    def s2(s):
        m = st[s]["m"]
        m[0].wait_recv()
        ring[s, 6] = acc[s, up(xa), :] + ring[s, 0]
        m.append(copy(ring.at[s, 6], ring.at[s, 4], right))
        m[1].wait_recv()
        ring[s, 7] = acc[s, down(xb), :] + ring[s, 1]
        m.append(copy(ring.at[s, 7], ring.at[s, 5], left))

    def s3(s):
        for m in st[s]["m"][2:]:
            m.wait_recv()
        acc[s, up(x), :] = acc[s, up(x), :] + (ring[s, 3] + ring[s, 4])
        acc[s, down(x), :] = acc[s, down(x), :] + (ring[s, 2] + ring[s, 5])
        st[s]["z"] = [copy(acc.at[(s,) + zpart(wz(z + d))], zb.at[s, d - 1], zs[d - 1]) for d in range(1, NZ)]

    def s4(s):
        for m in st[s]["z"]:
            m.wait_recv()
        r, l = zpart(z)
        t = acc[s, r, l]
        for d in range(NZ - 1):
            t = t + zb[s, d]
        t = t * scale
        zfin[s] = t
        r = rows_of(mine + x * pa + lax.div(z, 2) * zrow, zrow)
        st[s]["zz"] = [copy(zfin.at[s], fin.at[s, r, l], zs[d - 1]) for d in range(1, NZ)]
        fin[s, r, l] = t

    def s5(s):
        for m in st[s]["zz"]:
            m.wait_recv()
        f = lambda r: fin.at[s, r]
        fu = lambda q: f(rows_of(mine + q * pa, h))
        fd = lambda q: f(rows_of(mine + q * pa + h, h))
        st[s]["x"] = [
            copy(fu(x), fu(x), right), copy(fd(x), fd(x), left), copy(fd(x), fd(x), right), copy(fu(x), fu(x), left),
        ]
        whole = f(rows_of(mine + x * pa, pa))
        st[s]["o"] = [copy(whole, whole, other)]

    def s6(s):
        f = lambda r: fin.at[s, r]
        fu, fd = f(rows_of(mine + xb * pa, h)), f(rows_of(mine + xa * pa + h, h))
        m = st[s]["x"]
        m[0].wait_recv()
        m.append(copy(fu, fu, right))
        m[1].wait_recv()
        m.append(copy(fd, fd, left))

    def s7(s):
        m = st[s]["x"]
        m[2].wait_recv()
        m[3].wait_recv()
        for q in (xb, xa):
            whole = fin.at[s, rows_of(mine + q * pa, pa)]
            st[s]["o"].append(copy(whole, whole, other))
        m[4].wait_recv()
        m[5].wait_recv()
        whole = fin.at[s, rows_of(mine + xf * pa, pa)]
        st[s]["o"].append(copy(whole, whole, other))

    def s8(s):
        for m in st[s]["o"]:
            m.wait_recv()
        for i in range(2):
            to, frm = lanes_of(at[s][i], hp), pl.ds(i * hp, hp)
            block = fin[s, pl.ds(0, nq), frm]
            coeffs[:, to] = block
            ch[:, to], cl[:, to] = halves(block)
            pp[:, to] = fin[s, pl.ds(nq, npan), frm]

    rest = {}

    hq = hp // 4
    far_parts = {"a": [], "b": []}

    def far_sum(i):
        p = pl.ds(i * hq, hq)
        far_parts["a"].append(copy(s_ref.at[2, p], mid.at[0, p], north))
        far_parts["b"].append(copy(s_ref.at[2, pl.ds(hp + i * hq, hq)], mid.at[1, p], south))

    def near_sum():
        for m in far_parts["a"]:
            m.wait_recv()
        mid[6] = mid[0] + s_ref[3, pl.ds(hp, hp), :]
        rest["e"] = copy(mid.at[6], mid.at[4], north)
        for m in far_parts["b"]:
            m.wait_recv()
        mid[7] = mid[1] + s_ref[3, pl.ds(0, hp), :]
        rest["f"] = copy(mid.at[7], mid.at[5], south)

    def s9(s):
        t = dot3(halves(fin[s, pl.ds(0, nq), :]), (wh[pl.ds(0, nq)], wl[pl.ds(0, nq)]), TN)
        s_ref[s] = t
        lo, hi = s_ref.at[s, pl.ds(0, hp)], s_ref.at[s, pl.ds(hp, hp)]
        if s == 1:
            rest["c"] = copy(hi, mid.at[2], north)
            rest["d"] = copy(lo, mid.at[3], south)
        if s == 2:
            far_sum(0)
            far_sum(1)

    ng = part.shape[0]
    gq = ng // NY

    def g0():
        for u, rb in enumerate((x, 7 - x)):
            ct[...] = coeffs[:, lanes_of(rb * 128, 128)].T
            rs[pl.ds(u * 64, 64), pl.ds(0, nq)] = ct[rows_of(c * 64, 64), :]
        prod = dot3(halves(rs[:, pl.ds(0, nq)]), (ch[...], cl[...]), NN)
        rs[...] = prod
        for k in range(9):
            first = k < 8 - x
            rb = jnp.where(first, x, 7 - x)
            cb = jnp.where(first, x + k, k - 1)
            u = jnp.where(first, 0, 1)
            l = lanes_of(cb * 128, 128)
            own = (lax.div(rb, 2) == y).astype(F32)
            part[:, pl.ds(k * 128, 128)] = own * pp[rows_of(lax.rem(rb, 2) * 128 + c * 64, 64), l] - rs[rows_of(u * 64, 64), l]
        rest["r1"] = [copy(part.at[rows_of(wy(y + d) * gq, gq)], yb.at[d - 1], ys[d - 1]) for d in (2, 1, 3)]
        far_sum(3)

    gbase = c * (ng * NX)

    def g1():
        for m in rest["r1"]:
            m.wait_recv()
        t = part[rows_of(y * gq, gq)]
        for d in range(NY - 1):
            t = t + yb[d]
        gfin[...] = t
        to = rows_of(gbase + x * ng + y * gq, gq)
        rest["r2"] = [copy(gfin, g.at[to], ys[d - 1]) for d in (2, 1, 3)]
        g[to] = t
        near_sum()

    def summed():
        upper = lambda b: whole.at[rows_of(b * npan, hp)]
        lower = lambda b: whole.at[rows_of(b * npan + hp, hp)]
        same = lambda ref, to: plan(ref, ref, to)
        rest["d"].wait_recv()
        rest["e"].wait_recv()
        whole[rows_of(y * npan, hp)] = p_ref[pl.ds(0, hp)] - (s_ref[0, pl.ds(0, hp), :] + (mid[3] + mid[4]))
        early = [copy(upper(y), upper(y), north)]
        rest["c"].wait_recv()
        rest["f"].wait_recv()
        whole[rows_of(y * npan + hp, hp)] = p_ref[pl.ds(hp, hp)] - (s_ref[0, pl.ds(hp, hp), :] + (mid[2] + mid[5]))
        early.append(copy(lower(y), lower(y), south))
        rest["early"] = early
        rest["later"] = [copy(lower(y), lower(y), north), copy(upper(y), upper(y), south)]
        rest["pass_on"] = [same(upper(yb_), north), same(lower(ya), south)]

    def g2():
        for m in rest["r2"]:
            m.wait_recv()
        hg = ng // 2
        upper = lambda b: g.at[rows_of(gbase + b * ng, hg)]
        lower = lambda b: g.at[rows_of(gbase + b * ng + hg, hg)]
        whole_of = lambda b: g.at[rows_of(gbase + b * ng, ng)]
        m = [
            copy(upper(x), upper(x), right), copy(lower(x), lower(x), left),
            copy(lower(x), lower(x), right), copy(upper(x), upper(x), left),
        ]
        last = [copy(whole_of(x), whole_of(x), other)]
        m[0].wait_recv()
        m.append(copy(upper(xb), upper(xb), right))
        m[1].wait_recv()
        m.append(copy(lower(xa), lower(xa), left))
        m[2].wait_recv()
        last.append(copy(whole_of(xb), whole_of(xb), other))
        m[3].wait_recv()
        last.append(copy(whole_of(xa), whole_of(xa), other))
        m[4].wait_recv()
        m[5].wait_recv()
        last.append(copy(whole_of(xf), whole_of(xf), other))
        summed()
        for q in last:
            q.wait_recv()

    def s6_far(s):
        s6(s)
        if s == 3:
            far_sum(2)

    stages = (s0, s1, s2, s3, s4, s5, s6_far, s7, s8, s9)
    order = [(START[s] + AFTER[k], s, stages[k]) for s in range(4) for k in range(9)]
    order += [(START[s] + AFTER[8] + 0.1, s, s9) for s in range(3)]
    for _, s, stage in sorted(order, key=lambda e: e[:2]):
        stage(s)
    kept = pltpu.make_async_copy(coeffs, coeffs_hbm, done)
    kept.start()
    g0()
    s9(3)
    g1()
    g2()
    def split(b):
        r = rows_of(b * npan, npan)
        rh[r, :], rl[r, :] = halves(whole[r, :])

    later, pass_on = rest["later"], rest["pass_on"]

    def passed():
        for i in range(2):
            rest["early"][i].wait_recv()
            pass_on[i].start()

    def near():
        split(y)
        for m in later:
            m.wait_recv()
        split(yb_)
        split(ya)

    factorize(g, m_ref, th, tl, dict(zip(HOOKS, (passed, near))))
    mine_rows = m_ref[rows_of(y * npan, npan), :]
    total = mine_rows.shape[1]
    row = lax.broadcasted_iota(jnp.int32, (npan, total), 0) + y * npan
    col = lax.broadcasted_iota(jnp.int32, (npan, total), 1)
    xh, xl = halves(jnp.where(col <= row, mine_rows, 0.0))
    ch[pl.ds(0, npan)], cl[pl.ds(0, npan)] = xh, xl
    for m in pass_on:
        m.wait_recv()
    split(yf)

    def columns(i, _):
        l = lanes_of(i * 256, 256)
        out[:, l] = dot3((ch[pl.ds(0, npan)], cl[pl.ds(0, npan)]), (rh[:, l], rl[:, l]), NN)
        return 0

    lax.fori_loop(0, out.shape[1] // 256, columns, 0)
    kept.wait()
    for m in made:
        m.wait_send()


HOOKS = (2, 5)
START = (3.0, 13.0, 24.5, 36.0)
AFTER = (0.0, 2.0, 5.0, 8.0, 15.0, 22.0, 25.0, 28.0, 30.0)


def step(basis, panel, scale):
    nq, w = basis.shape
    npan = panel.shape[0]
    total = npan * NY
    n = nq + npan
    half = n // 2
    pa = half // NX
    hp = npan // 2
    space = pl.BlockSpec(memory_space=pltpu.VMEM)
    short = [(n, w), (n, w), (nq, total), (nq, total)] + [(B, total + SPARE * B)] * 2 + [(total, w)] * 2
    shapes = [
        (6, hp, w), (4, n, 2 * hp), (4, half, 2 * hp), (4, half, 2 * hp), (4, 8, pa // 2, 2 * hp),
        (4, NZ - 1, pa * 2 // NZ, 128), (4, pa * 2 // NZ, 128), (4, n, 2 * hp),
        (npan, total), (128, nq), (128, total), (64, 9 * 128), (4, npan, w), (512, 9 * 128), (total + SPARE * B, total),
        (NY - 1, 64 // NY, 9 * 128), (64 // NY, 9 * 128), (8, hp, w), (total, w), (nq, total),
    ]
    copies = 6 + 4 * (1 + 6 + 7 + 7 + 6 + 4) + 36
    return pl.pallas_call(
        functools.partial(step_kernel, scale),
        name="step",
        out_shape=[jax.ShapeDtypeStruct((npan, w), F32), jax.ShapeDtypeStruct((nq, total), F32)],
        in_specs=[space] * 2,
        out_specs=[space, pl.BlockSpec(memory_space=pl.ANY)],
        scratch_shapes=[pltpu.VMEM(s_, BF16) for s_ in short] + [pltpu.VMEM(s_, F32) for s_ in shapes]
        + [pltpu.SemaphoreType.DMA((copies,)), pltpu.SemaphoreType.DMA((copies,)), pltpu.SemaphoreType.DMA(())],
        compiler_params=pltpu.CompilerParams(collective_id=1, has_side_effects=True, vmem_limit_bytes=60 * 2**20),
    )(basis, panel)


def body(basis, panel):
    n_grid = panel.shape[1] * lax.axis_size("grid")
    return tuple(step(basis, panel, 1.0 / n_grid))


def solution(mesh):
    placed = (P("band", "grid"), P("band", "grid"))
    return jax.shard_map(
        body, mesh=mesh, in_specs=placed, out_specs=(P("band", "grid"), P("band", None)), check_vma=False,
    )
```

```python
import functools

import jax
import jax.numpy as jnp
from jax import lax
from jax.experimental import pallas as pl
from jax.experimental.pallas import tpu as pltpu
from jax.sharding import PartitionSpec as P

F32, BF16 = jnp.float32, jnp.bfloat16

def halves(x):
    hi = x.astype(BF16)
    return hi, (x - hi.astype(F32)).astype(BF16)

def dot3(a, b, dims):
    (ah, al), (bh, bl) = a, b
    dg = lambda u, v: lax.dot_general(u, v, (dims, ((), ())), preferred_element_type=F32)
    return dg(ah, bh) + (dg(ah, bl) + dg(al, bh))

NN, TN, NT = ((1,), (0,)), ((0,), (0,)), ((1,), (1,))
BASE = 32

def base_block(w, at):
    n = w.shape[0]
    rows = w[at:at + BASE]
    lane = lax.broadcasted_iota(jnp.int32, (BASE, n), 1)
    sub = lax.broadcasted_iota(jnp.int32, (BASE, n), 0)
    cols = []
    for j in range(BASE):
        lo = j // 8 * 8
        cols.append(jnp.broadcast_to(rows[lo:, at + j:at + j + 1], (BASE - lo, n)))
    inside = (lane >= at) & (lane < at + BASE)
    v = jnp.where(inside, (lane == sub + at).astype(F32), rows)
    v = [v[8 * s:8 * s + 8] for s in range(BASE // 8)]
    cols = [[c[8 * s:8 * s + 8] for s in range(c.shape[0] // 8)] for c in cols]
    nb = BASE // 8
    sub8 = lax.broadcasted_iota(jnp.int32, (8, n), 0)
    bc = lambda x, i: jnp.broadcast_to(x[i:i + 1], (8, n))
    for j in range(BASE):
        s0, r0 = j // 8, j % 8
        c = cols[j]
        inv = lax.rsqrt(bc(c[0], r0))
        l = [x * inv for x in c]
        for jj in range(j + 1, BASE):
            s1, r1 = jj // 8, jj % 8
            f = bc(l[s1 - s0], r1)
            for s in range(s1, nb):
                cols[jj][s - s1] = cols[jj][s - s1] - l[s - s0] * f
        piv = bc(v[s0], r0) * inv
        l0 = jnp.where(sub8 > r0, l[0], 0.0)
        v[s0] = jnp.where(sub8 == r0, piv, v[s0] - l0 * piv)
        for s in range(s0 + 1, nb):
            v[s] = v[s] - l[s - s0] * piv
    return jnp.concatenate(v, 0)

def factor128(w):
    n = w.shape[0]
    lane = lax.broadcasted_iota(jnp.int32, (n, n), 1)
    row = lax.broadcasted_iota(jnp.int32, (n, n), 0)
    for at in range(0, n, BASE):
        v = base_block(w, at)
        end = at + BASE
        if end < n:
            parts = halves(v)
            upd = dot3(parts, parts, TN)
            below = w[end:]
            l2 = lane[end:]
            below = jnp.where((l2 >= at) & (l2 < end), 0.0, below) - upd[end:]
            w = jnp.concatenate(([w[:at]] if at else []) + [v, below], 0)
        else:
            w = jnp.concatenate([w[:at], v], 0)
    return jnp.where(lane <= row, w, 0.0)

B = 128


SEGMENTS = ((0, 1, 0), (1, 4, 6), (4, 8, 3))
SPARE = 4


def factorize(g_ref, m_ref, th, tl, between):
    n = m_ref.shape[1]
    nb = n // B
    hb = g_ref.shape[0] // 2
    for t in range(nb // 2):
        for c in range(2):
            src = pl.ds(c * hb + t * 64, 64)
            m_ref[pl.ds(t * B + c * 64, 64), pl.ds(t * B, n - t * B)] = g_ref[src, pl.ds(0, n - t * B)]
            u = nb - 1 - t
            m_ref[pl.ds(u * B + c * 64, 64), pl.ds(u * B, n - u * B)] = g_ref[src, pl.ds(n - t * B, n - u * B)]
    th[:, pl.ds(n, SPARE * B)] = jnp.zeros((B, SPARE * B), BF16)
    tl[:, pl.ds(n, SPARE * B)] = jnp.zeros((B, SPARE * B), BF16)
    block = lambda i, count=1: pl.ds(pl.multiple_of(i * B, B), count * B)

    def update(i, count, k):
        q = block(i, count)
        m_ref[q, block(k)] = jnp.zeros((count * B, B), F32)
        m_ref[q, :] = m_ref[q, :] - dot3((th[:, q], tl[:, q]), (th[:, :n], tl[:, :n]), TN)

    def step(acts, count, k, _):
        inv = factor128(m_ref[block(k), block(k)])
        if count:
            update(k + 1, count, k - 1)
        t = dot3(halves(inv), halves(m_ref[block(k), :]), NN)
        m_ref[block(k), :] = t
        m_ref[block(k), block(k)] = inv
        hi, lo = halves(m_ref[block(k), :])
        th[:, :n] = hi
        tl[:, :n] = lo
        update(k + 1, 1, k)
        for when, act in acts.items():
            pl.when(k == when)(act)
        return 0

    for a, z, count in SEGMENTS:
        acts = {k: act for k, act in between.items() if a <= k < z}
        lax.fori_loop(a, z, functools.partial(step, acts, count), 0)


MESH = pl.DeviceIdType.MESH
NX, NZ, NY = 4, 8, 4


def place():
    g = lax.axis_index("grid")
    return lax.rem(g, 2), lax.rem(lax.div(g, 2), NX), lax.div(g, 2 * NX), lax.axis_index("band")


def grid_id(z, x, c):
    return {"grid": (z * NX + x) * 2 + c}


def sender(send, recv):
    made = []

    def plan(src, dst, device):
        at = len(made)
        made.append(
            pltpu.make_async_remote_copy(
                src_ref=src, dst_ref=dst, send_sem=send.at[at], recv_sem=recv.at[at],
                device_id=device, device_id_type=MESH,
            )
        )
        return made[-1]

    def copy(src, dst, device):
        started = plan(src, dst, device)
        started.start()
        return started

    return plan, copy, made


def greet(devices):
    barrier = pltpu.get_barrier_semaphore()
    for device in devices:
        pl.semaphore_signal(barrier, inc=1, device_id=device, device_id_type=MESH)
    pl.semaphore_wait(barrier, len(devices))


def rows_of(start, count):
    return pl.ds(pl.multiple_of(start, 8), count)


def lanes_of(start, count):
    return pl.ds(pl.multiple_of(start, 128), count)


def step_kernel(
    scale, q_ref, p_ref, out, coeffs_hbm, wh, wl, ch, cl, th, tl, rh, rl, pg, v, pair, acc, ring, zb, zfin, fin,
    pp, ct, rs, part, s_ref, g, m_ref, yb, gfin, mid, whole, coeffs, send, recv, done,
):
    c, x, z, y = place()
    nq, npan = q_ref.shape[0], p_ref.shape[0]
    half = v.shape[1] // 2
    pa = half // NX
    h = pa // 2
    zrow = pa // (NZ // 2)
    wx, wz, wy = (lambda q: lax.rem(q, NX)), (lambda q: lax.rem(q, NZ)), (lambda q: lax.rem(q, NY))
    other = grid_id(z, x, 1 - c)
    right, left = grid_id(z, wx(x + 1), c), grid_id(z, wx(x + NX - 1), c)
    zs = [grid_id(wz(z + d), x, c) for d in range(1, NZ)]
    north, south = {"band": wy(y + 1)}, {"band": wy(y + NY - 1)}
    ys = [{"band": lax.rem(y + d, NY)} for d in range(1, NY)]
    greet([other, right, left] + ys + zs)
    plan, copy, made = sender(send, recv)
    mine, theirs = c * half, (1 - c) * half
    xb, xa, xf = wx(x + NX - 1), wx(x + 1), wx(x + 2)
    yb_, ya, yf = wy(y + NY - 1), wy(y + 1), wy(y + 2)
    hp = npan // 2
    p1, p2 = p_ref.at[pl.ds(0, hp)], p_ref.at[pl.ds(hp, hp)]
    lead, tail = pl.ds(0, hp // 4), pl.ds(hp // 4, hp - hp // 4)
    gs = [
        copy(p1, pg.at[0], north), copy(p2, pg.at[1], south),
        copy(p2.at[lead], pg.at[2, lead], north), copy(p1.at[lead], pg.at[3, lead], south),
    ]
    at = [
        (y * npan, y * npan + hp), (yb_ * npan, ya * npan + hp),
        (yf * npan, yf * npan + hp), (yb_ * npan + hp, ya * npan),
    ]
    wh[pl.ds(0, nq)], wl[pl.ds(0, nq)] = halves(q_ref[...])
    wh[pl.ds(nq, npan)], wl[pl.ds(nq, npan)] = halves(p_ref[...])
    n = wh.shape[0]
    tile = 256

    def product(s, rows):
        ph, plo = halves(rows)

        def some(i, _):
            r = rows_of(i * tile, tile)
            v[s, r, :] = dot3((wh[r, :], wl[r, :]), (ph, plo), NT)
            return 0

        lax.fori_loop(0, n // tile, some, 0)

    st = [dict() for _ in range(4)]
    piece = lambda q: rows_of(q * pa, pa)
    up = lambda q: rows_of(q * pa, h)
    down = lambda q: rows_of(q * pa + h, h)
    zpart = lambda q: (rows_of(x * pa + lax.div(q, 2) * zrow, zrow), lanes_of(lax.rem(q, 2) * 128, 128))

    def s0(s):
        if s == 0:
            product(0, p_ref[...])
        else:
            if s == 1:
                gs[0].wait_recv()
                gs.append(copy(pg.at[0], pg.at[4], north))
                gs.append(copy(p2.at[tail], pg.at[2, tail], north))
                gs[1].wait_recv()
                gs.append(copy(pg.at[1], pg.at[5], south))
                gs.append(copy(p1.at[tail], pg.at[3, tail], south))
            for m in {1: (), 2: (4, 6), 3: (2, 3, 5, 7)}[s]:
                gs[m].wait_recv()
            u = {1: 0, 2: 4, 3: 2}[s]
            product(s, jnp.concatenate([pg[u], pg[u + 1]], 0))
        st[s]["pair"] = copy(v.at[s, rows_of(theirs, half)], pair.at[s], other)

    def s1(s):
        st[s]["pair"].wait_recv()
        acc[s] = v[s, rows_of(mine, half), :] + pair[s]
        st[s]["m"] = [
            copy(acc.at[s, up(xf)], ring.at[s, 0], right), copy(acc.at[s, down(xf)], ring.at[s, 1], left),
            copy(acc.at[s, down(xa)], ring.at[s, 2], right), copy(acc.at[s, up(xb)], ring.at[s, 3], left),
        ]

    def s2(s):
        m = st[s]["m"]
        m[0].wait_recv()
        ring[s, 6] = acc[s, up(xa), :] + ring[s, 0]
        m.append(copy(ring.at[s, 6], ring.at[s, 4], right))
        m[1].wait_recv()
        ring[s, 7] = acc[s, down(xb), :] + ring[s, 1]
        m.append(copy(ring.at[s, 7], ring.at[s, 5], left))

    def s3(s):
        for m in st[s]["m"][2:]:
            m.wait_recv()
        acc[s, up(x), :] = acc[s, up(x), :] + (ring[s, 3] + ring[s, 4])
        acc[s, down(x), :] = acc[s, down(x), :] + (ring[s, 2] + ring[s, 5])
        st[s]["z"] = [copy(acc.at[(s,) + zpart(wz(z + d))], zb.at[s, d - 1], zs[d - 1]) for d in range(1, NZ)]

    def s4(s):
        for m in st[s]["z"]:
            m.wait_recv()
        r, l = zpart(z)
        t = acc[s, r, l]
        for d in range(NZ - 1):
            t = t + zb[s, d]
        t = t * scale
        zfin[s] = t
        r = rows_of(mine + x * pa + lax.div(z, 2) * zrow, zrow)
        st[s]["zz"] = [copy(zfin.at[s], fin.at[s, r, l], zs[d - 1]) for d in range(1, NZ)]
        fin[s, r, l] = t

    def s5(s):
        for m in st[s]["zz"]:
            m.wait_recv()
        f = lambda r: fin.at[s, r]
        fu = lambda q: f(rows_of(mine + q * pa, h))
        fd = lambda q: f(rows_of(mine + q * pa + h, h))
        st[s]["x"] = [
            copy(fu(x), fu(x), right), copy(fd(x), fd(x), left), copy(fd(x), fd(x), right), copy(fu(x), fu(x), left),
        ]
        whole = f(rows_of(mine + x * pa, pa))
        st[s]["o"] = [copy(whole, whole, other)]

    def s6(s):
        f = lambda r: fin.at[s, r]
        fu, fd = f(rows_of(mine + xb * pa, h)), f(rows_of(mine + xa * pa + h, h))
        m = st[s]["x"]
        m[0].wait_recv()
        m.append(copy(fu, fu, right))
        m[1].wait_recv()
        m.append(copy(fd, fd, left))

    def s7(s):
        m = st[s]["x"]
        m[2].wait_recv()
        m[3].wait_recv()
        for q in (xb, xa):
            whole = fin.at[s, rows_of(mine + q * pa, pa)]
            st[s]["o"].append(copy(whole, whole, other))
        m[4].wait_recv()
        m[5].wait_recv()
        whole = fin.at[s, rows_of(mine + xf * pa, pa)]
        st[s]["o"].append(copy(whole, whole, other))

    def s8(s):
        for m in st[s]["o"]:
            m.wait_recv()
        for i in range(2):
            to, frm = lanes_of(at[s][i], hp), pl.ds(i * hp, hp)
            block = fin[s, pl.ds(0, nq), frm]
            coeffs[:, to] = block
            ch[:, to], cl[:, to] = halves(block)
            pp[:, to] = fin[s, pl.ds(nq, npan), frm]

    rest = {}

    hq = hp // 4
    far_parts = {"a": [], "b": []}

    def far_sum(i):
        p = pl.ds(i * hq, hq)
        far_parts["a"].append(copy(s_ref.at[2, p], mid.at[0, p], north))
        far_parts["b"].append(copy(s_ref.at[2, pl.ds(hp + i * hq, hq)], mid.at[1, p], south))

    def near_sum():
        for m in far_parts["a"]:
            m.wait_recv()
        mid[6] = mid[0] + s_ref[3, pl.ds(hp, hp), :]
        rest["e"] = copy(mid.at[6], mid.at[4], north)
        for m in far_parts["b"]:
            m.wait_recv()
        mid[7] = mid[1] + s_ref[3, pl.ds(0, hp), :]
        rest["f"] = copy(mid.at[7], mid.at[5], south)

    def s9(s):
        t = dot3(halves(fin[s, pl.ds(0, nq), :]), (wh[pl.ds(0, nq)], wl[pl.ds(0, nq)]), TN)
        s_ref[s] = t
        lo, hi = s_ref.at[s, pl.ds(0, hp)], s_ref.at[s, pl.ds(hp, hp)]
        if s == 1:
            rest["c"] = copy(hi, mid.at[2], north)
            rest["d"] = copy(lo, mid.at[3], south)
        if s == 2:
            far_sum(0)
            far_sum(1)

    ng = part.shape[0]
    gq = ng // NY

    def g0():
        for u, rb in enumerate((x, 7 - x)):
            ct[...] = coeffs[:, lanes_of(rb * 128, 128)].T
            rs[pl.ds(u * 64, 64), pl.ds(0, nq)] = ct[rows_of(c * 64, 64), :]
        prod = dot3(halves(rs[:, pl.ds(0, nq)]), (ch[...], cl[...]), NN)
        rs[...] = prod
        for k in range(9):
            first = k < 8 - x
            rb = jnp.where(first, x, 7 - x)
            cb = jnp.where(first, x + k, k - 1)
            u = jnp.where(first, 0, 1)
            l = lanes_of(cb * 128, 128)
            own = (lax.div(rb, 2) == y).astype(F32)
            part[:, pl.ds(k * 128, 128)] = own * pp[rows_of(lax.rem(rb, 2) * 128 + c * 64, 64), l] - rs[rows_of(u * 64, 64), l]
        rest["r1"] = [copy(part.at[rows_of(wy(y + d) * gq, gq)], yb.at[d - 1], ys[d - 1]) for d in (2, 1, 3)]
        far_sum(3)

    gbase = c * (ng * NX)

    def g1():
        for m in rest["r1"]:
            m.wait_recv()
        t = part[rows_of(y * gq, gq)]
        for d in range(NY - 1):
            t = t + yb[d]
        gfin[...] = t
        to = rows_of(gbase + x * ng + y * gq, gq)
        rest["r2"] = [copy(gfin, g.at[to], ys[d - 1]) for d in (2, 1, 3)]
        g[to] = t
        near_sum()

    def summed():
        upper = lambda b: whole.at[rows_of(b * npan, hp)]
        lower = lambda b: whole.at[rows_of(b * npan + hp, hp)]
        same = lambda ref, to: plan(ref, ref, to)
        rest["d"].wait_recv()
        rest["e"].wait_recv()
        whole[rows_of(y * npan, hp)] = p_ref[pl.ds(0, hp)] - (s_ref[0, pl.ds(0, hp), :] + (mid[3] + mid[4]))
        early = [copy(upper(y), upper(y), north)]
        rest["c"].wait_recv()
        rest["f"].wait_recv()
        whole[rows_of(y * npan + hp, hp)] = p_ref[pl.ds(hp, hp)] - (s_ref[0, pl.ds(hp, hp), :] + (mid[2] + mid[5]))
        early.append(copy(lower(y), lower(y), south))
        rest["early"] = early
        rest["later"] = [copy(lower(y), lower(y), north), copy(upper(y), upper(y), south)]
        rest["pass_on"] = [same(upper(yb_), north), same(lower(ya), south)]

    def g2():
        for m in rest["r2"]:
            m.wait_recv()
        hg = ng // 2
        upper = lambda b: g.at[rows_of(gbase + b * ng, hg)]
        lower = lambda b: g.at[rows_of(gbase + b * ng + hg, hg)]
        whole_of = lambda b: g.at[rows_of(gbase + b * ng, ng)]
        m = [
            copy(upper(x), upper(x), right), copy(lower(x), lower(x), left),
            copy(lower(x), lower(x), right), copy(upper(x), upper(x), left),
        ]
        last = [copy(whole_of(x), whole_of(x), other)]
        m[0].wait_recv()
        m.append(copy(upper(xb), upper(xb), right))
        m[1].wait_recv()
        m.append(copy(lower(xa), lower(xa), left))
        m[2].wait_recv()
        last.append(copy(whole_of(xb), whole_of(xb), other))
        m[3].wait_recv()
        last.append(copy(whole_of(xa), whole_of(xa), other))
        m[4].wait_recv()
        m[5].wait_recv()
        last.append(copy(whole_of(xf), whole_of(xf), other))
        summed()
        for q in last:
            q.wait_recv()

    def s6_far(s):
        s6(s)
        if s == 3:
            far_sum(2)

    stages = (s0, s1, s2, s3, s4, s5, s6_far, s7, s8, s9)
    order = [(START[s] + AFTER[k], s, stages[k]) for s in range(4) for k in range(9)]
    order += [(START[s] + AFTER[8] + 0.1, s, s9) for s in (1, 2)]
    for _, s, stage in sorted(order, key=lambda e: e[:2]):
        stage(s)
    kept = pltpu.make_async_copy(coeffs, coeffs_hbm, done)
    kept.start()
    g0()
    s9(3)
    s9(0)
    g1()
    g2()
    def split(b):
        r = rows_of(b * npan, npan)
        rh[r, :], rl[r, :] = halves(whole[r, :])

    later, pass_on = rest["later"], rest["pass_on"]

    def passed():
        for i in range(2):
            rest["early"][i].wait_recv()
            pass_on[i].start()

    def near():
        split(y)
        for m in later:
            m.wait_recv()
        split(yb_)
        split(ya)

    factorize(g, m_ref, th, tl, dict(zip(HOOKS, (passed, near))))
    mine_rows = m_ref[rows_of(y * npan, npan), :]
    total = mine_rows.shape[1]
    row = lax.broadcasted_iota(jnp.int32, (npan, total), 0) + y * npan
    col = lax.broadcasted_iota(jnp.int32, (npan, total), 1)
    xh, xl = halves(jnp.where(col <= row, mine_rows, 0.0))
    ch[pl.ds(0, npan)], cl[pl.ds(0, npan)] = xh, xl
    for m in pass_on:
        m.wait_recv()
    split(yf)

    def columns(i, _):
        l = lanes_of(i * 256, 256)
        out[:, l] = dot3((ch[pl.ds(0, npan)], cl[pl.ds(0, npan)]), (rh[:, l], rl[:, l]), NN)
        return 0

    lax.fori_loop(0, out.shape[1] // 256, columns, 0)
    kept.wait()
    for m in made:
        m.wait_send()


HOOKS = (2, 5)
START = (3.0, 13.0, 27.0, 34.5)
AFTER = (0.0, 2.0, 5.0, 8.0, 15.0, 22.0, 25.0, 28.0, 32.0)


def step(basis, panel, scale):
    nq, w = basis.shape
    npan = panel.shape[0]
    total = npan * NY
    n = nq + npan
    half = n // 2
    pa = half // NX
    hp = npan // 2
    space = pl.BlockSpec(memory_space=pltpu.VMEM)
    short = [(n, w), (n, w), (nq, total), (nq, total)] + [(B, total + SPARE * B)] * 2 + [(total, w)] * 2
    shapes = [
        (6, hp, w), (4, n, 2 * hp), (4, half, 2 * hp), (4, half, 2 * hp), (4, 8, pa // 2, 2 * hp),
        (4, NZ - 1, pa * 2 // NZ, 128), (4, pa * 2 // NZ, 128), (4, n, 2 * hp),
        (npan, total), (128, nq), (128, total), (64, 9 * 128), (4, npan, w), (512, 9 * 128), (total + SPARE * B, total),
        (NY - 1, 64 // NY, 9 * 128), (64 // NY, 9 * 128), (8, hp, w), (total, w), (nq, total),
    ]
    copies = 6 + 4 * (1 + 6 + 7 + 7 + 6 + 4) + 36
    return pl.pallas_call(
        functools.partial(step_kernel, scale),
        name="step",
        out_shape=[jax.ShapeDtypeStruct((npan, w), F32), jax.ShapeDtypeStruct((nq, total), F32)],
        in_specs=[space] * 2,
        out_specs=[space, pl.BlockSpec(memory_space=pl.ANY)],
        scratch_shapes=[pltpu.VMEM(s_, BF16) for s_ in short] + [pltpu.VMEM(s_, F32) for s_ in shapes]
        + [pltpu.SemaphoreType.DMA((copies,)), pltpu.SemaphoreType.DMA((copies,)), pltpu.SemaphoreType.DMA(())],
        compiler_params=pltpu.CompilerParams(collective_id=1, has_side_effects=True, vmem_limit_bytes=60 * 2**20),
    )(basis, panel)


def body(basis, panel):
    n_grid = panel.shape[1] * lax.axis_size("grid")
    return tuple(step(basis, panel, 1.0 / n_grid))


def solution(mesh):
    placed = (P("band", "grid"), P("band", "grid"))
    return jax.shard_map(
        body, mesh=mesh, in_specs=placed, out_specs=(P("band", "grid"), P("band", None)), check_vma=False,
    )
```

```python
import functools

import jax
import jax.numpy as jnp
from jax import lax
from jax.experimental import pallas as pl
from jax.experimental.pallas import tpu as pltpu
from jax.sharding import PartitionSpec as P

F32, BF16 = jnp.float32, jnp.bfloat16

def halves(x):
    hi = x.astype(BF16)
    return hi, (x - hi.astype(F32)).astype(BF16)

def dot3(a, b, dims):
    (ah, al), (bh, bl) = a, b
    dg = lambda u, v: lax.dot_general(u, v, (dims, ((), ())), preferred_element_type=F32)
    return dg(ah, bh) + (dg(ah, bl) + dg(al, bh))

NN, TN, NT = ((1,), (0,)), ((0,), (0,)), ((1,), (1,))
BASE = 32

def base_block(w, at):
    n = w.shape[0]
    rows = w[at:at + BASE]
    lane = lax.broadcasted_iota(jnp.int32, (BASE, n), 1)
    sub = lax.broadcasted_iota(jnp.int32, (BASE, n), 0)
    cols = []
    for j in range(BASE):
        lo = j // 8 * 8
        cols.append(jnp.broadcast_to(rows[lo:, at + j:at + j + 1], (BASE - lo, n)))
    inside = (lane >= at) & (lane < at + BASE)
    v = jnp.where(inside, (lane == sub + at).astype(F32), rows)
    v = [v[8 * s:8 * s + 8] for s in range(BASE // 8)]
    cols = [[c[8 * s:8 * s + 8] for s in range(c.shape[0] // 8)] for c in cols]
    nb = BASE // 8
    sub8 = lax.broadcasted_iota(jnp.int32, (8, n), 0)
    bc = lambda x, i: jnp.broadcast_to(x[i:i + 1], (8, n))
    for j in range(BASE):
        s0, r0 = j // 8, j % 8
        c = cols[j]
        inv = lax.rsqrt(bc(c[0], r0))
        l = [x * inv for x in c]
        for jj in range(j + 1, BASE):
            s1, r1 = jj // 8, jj % 8
            f = bc(l[s1 - s0], r1)
            for s in range(s1, nb):
                cols[jj][s - s1] = cols[jj][s - s1] - l[s - s0] * f
        piv = bc(v[s0], r0) * inv
        l0 = jnp.where(sub8 > r0, l[0], 0.0)
        v[s0] = jnp.where(sub8 == r0, piv, v[s0] - l0 * piv)
        for s in range(s0 + 1, nb):
            v[s] = v[s] - l[s - s0] * piv
    return jnp.concatenate(v, 0)

def factor128(w):
    n = w.shape[0]
    lane = lax.broadcasted_iota(jnp.int32, (n, n), 1)
    row = lax.broadcasted_iota(jnp.int32, (n, n), 0)
    for at in range(0, n, BASE):
        v = base_block(w, at)
        end = at + BASE
        if end < n:
            parts = halves(v)
            upd = dot3(parts, parts, TN)
            below = w[end:]
            l2 = lane[end:]
            below = jnp.where((l2 >= at) & (l2 < end), 0.0, below) - upd[end:]
            w = jnp.concatenate(([w[:at]] if at else []) + [v, below], 0)
        else:
            w = jnp.concatenate([w[:at], v], 0)
    return jnp.where(lane <= row, w, 0.0)

B = 128


SEGMENTS = ((0, 1, 0), (1, 4, 6), (4, 8, 3))
SPARE = 4


def factorize(g_ref, m_ref, th, tl, between):
    n = m_ref.shape[1]
    nb = n // B
    hb = g_ref.shape[0] // 2
    for t in range(nb // 2):
        for c in range(2):
            src = pl.ds(c * hb + t * 64, 64)
            m_ref[pl.ds(t * B + c * 64, 64), pl.ds(t * B, n - t * B)] = g_ref[src, pl.ds(0, n - t * B)]
            u = nb - 1 - t
            m_ref[pl.ds(u * B + c * 64, 64), pl.ds(u * B, n - u * B)] = g_ref[src, pl.ds(n - t * B, n - u * B)]
    th[:, pl.ds(n, SPARE * B)] = jnp.zeros((B, SPARE * B), BF16)
    tl[:, pl.ds(n, SPARE * B)] = jnp.zeros((B, SPARE * B), BF16)
    block = lambda i, count=1: pl.ds(pl.multiple_of(i * B, B), count * B)

    def update(i, count, k):
        q = block(i, count)
        m_ref[q, block(k)] = jnp.zeros((count * B, B), F32)
        m_ref[q, :] = m_ref[q, :] - dot3((th[:, q], tl[:, q]), (th[:, :n], tl[:, :n]), TN)

    def step(acts, count, k, _):
        inv = factor128(m_ref[block(k), block(k)])
        if count:
            update(k + 1, count, k - 1)
        t = dot3(halves(inv), halves(m_ref[block(k), :]), NN)
        m_ref[block(k), :] = t
        m_ref[block(k), block(k)] = inv
        hi, lo = halves(m_ref[block(k), :])
        th[:, :n] = hi
        tl[:, :n] = lo
        update(k + 1, 1, k)
        for when, act in acts.items():
            pl.when(k == when)(act)
        return 0

    for a, z, count in SEGMENTS:
        acts = {k: act for k, act in between.items() if a <= k < z}
        lax.fori_loop(a, z, functools.partial(step, acts, count), 0)


MESH = pl.DeviceIdType.MESH
NX, NZ, NY = 4, 8, 4


def place():
    g = lax.axis_index("grid")
    return lax.rem(g, 2), lax.rem(lax.div(g, 2), NX), lax.div(g, 2 * NX), lax.axis_index("band")


def grid_id(z, x, c):
    return {"grid": (z * NX + x) * 2 + c}


def sender(send, recv):
    made = []

    def plan(src, dst, device):
        at = len(made)
        made.append(
            pltpu.make_async_remote_copy(
                src_ref=src, dst_ref=dst, send_sem=send.at[at], recv_sem=recv.at[at],
                device_id=device, device_id_type=MESH,
            )
        )
        return made[-1]

    def copy(src, dst, device):
        started = plan(src, dst, device)
        started.start()
        return started

    return plan, copy, made


def greet(devices):
    barrier = pltpu.get_barrier_semaphore()
    for device in devices:
        pl.semaphore_signal(barrier, inc=1, device_id=device, device_id_type=MESH)
    pl.semaphore_wait(barrier, len(devices))


def rows_of(start, count):
    return pl.ds(pl.multiple_of(start, 8), count)


def lanes_of(start, count):
    return pl.ds(pl.multiple_of(start, 128), count)


def step_kernel(
    scale, q_ref, p_ref, out, coeffs_hbm, wh, wl, ch, cl, th, tl, rh, rl, pg, v, pair, acc, ring, zb, zfin, fin,
    pp, ct, rs, part, s_ref, g, m_ref, yb, gfin, mid, whole, coeffs, send, recv, done,
):
    c, x, z, y = place()
    nq, npan = q_ref.shape[0], p_ref.shape[0]
    half = v.shape[1] // 2
    pa = half // NX
    h = pa // 2
    zrow = pa // (NZ // 2)
    wx, wz, wy = (lambda q: lax.rem(q, NX)), (lambda q: lax.rem(q, NZ)), (lambda q: lax.rem(q, NY))
    other = grid_id(z, x, 1 - c)
    right, left = grid_id(z, wx(x + 1), c), grid_id(z, wx(x + NX - 1), c)
    zs = [grid_id(wz(z + d), x, c) for d in range(1, NZ)]
    north, south = {"band": wy(y + 1)}, {"band": wy(y + NY - 1)}
    ys = [{"band": lax.rem(y + d, NY)} for d in range(1, NY)]
    greet([other, right, left] + ys + zs)
    plan, copy, made = sender(send, recv)
    mine, theirs = c * half, (1 - c) * half
    xb, xa, xf = wx(x + NX - 1), wx(x + 1), wx(x + 2)
    yb_, ya, yf = wy(y + NY - 1), wy(y + 1), wy(y + 2)
    hp = npan // 2
    p1, p2 = p_ref.at[pl.ds(0, hp)], p_ref.at[pl.ds(hp, hp)]
    lead, tail = pl.ds(0, hp // 4), pl.ds(hp // 4, hp - hp // 4)
    gs = [
        copy(p1, pg.at[0], north), copy(p2, pg.at[1], south),
        copy(p2.at[lead], pg.at[2, lead], north), copy(p1.at[lead], pg.at[3, lead], south),
    ]
    at = [
        (y * npan, y * npan + hp), (yb_ * npan, ya * npan + hp),
        (yf * npan, yf * npan + hp), (yb_ * npan + hp, ya * npan),
    ]
    wh[pl.ds(0, nq)], wl[pl.ds(0, nq)] = halves(q_ref[...])
    wh[pl.ds(nq, npan)], wl[pl.ds(nq, npan)] = halves(p_ref[...])
    n = wh.shape[0]
    tile = 256

    def product(s, rows):
        ph, plo = halves(rows)

        def some(i, _):
            r = rows_of(i * tile, tile)
            v[s, r, :] = dot3((wh[r, :], wl[r, :]), (ph, plo), NT)
            return 0

        lax.fori_loop(0, n // tile, some, 0)

    st = [dict() for _ in range(4)]
    piece = lambda q: rows_of(q * pa, pa)
    up = lambda q: rows_of(q * pa, h)
    down = lambda q: rows_of(q * pa + h, h)
    zpart = lambda q: (rows_of(x * pa + lax.div(q, 2) * zrow, zrow), lanes_of(lax.rem(q, 2) * 128, 128))

    def s0(s):
        if s == 0:
            product(0, p_ref[...])
        else:
            if s == 1:
                gs[0].wait_recv()
                gs.append(copy(pg.at[0], pg.at[4], north))
                gs.append(copy(p2.at[tail], pg.at[2, tail], north))
                gs[1].wait_recv()
                gs.append(copy(pg.at[1], pg.at[5], south))
                gs.append(copy(p1.at[tail], pg.at[3, tail], south))
            for m in {1: (), 2: (4, 6), 3: (2, 3, 5, 7)}[s]:
                gs[m].wait_recv()
            u = {1: 0, 2: 4, 3: 2}[s]
            product(s, jnp.concatenate([pg[u], pg[u + 1]], 0))
        st[s]["pair"] = copy(v.at[s, rows_of(theirs, half)], pair.at[s], other)

    def s1(s):
        st[s]["pair"].wait_recv()
        acc[s] = v[s, rows_of(mine, half), :] + pair[s]
        st[s]["m"] = [
            copy(acc.at[s, up(xf)], ring.at[s, 0], right), copy(acc.at[s, down(xf)], ring.at[s, 1], left),
            copy(acc.at[s, down(xa)], ring.at[s, 2], right), copy(acc.at[s, up(xb)], ring.at[s, 3], left),
        ]

    def s2(s):
        m = st[s]["m"]
        m[0].wait_recv()
        ring[s, 6] = acc[s, up(xa), :] + ring[s, 0]
        m.append(copy(ring.at[s, 6], ring.at[s, 4], right))
        m[1].wait_recv()
        ring[s, 7] = acc[s, down(xb), :] + ring[s, 1]
        m.append(copy(ring.at[s, 7], ring.at[s, 5], left))

    def s3(s):
        for m in st[s]["m"][2:]:
            m.wait_recv()
        acc[s, up(x), :] = acc[s, up(x), :] + (ring[s, 3] + ring[s, 4])
        acc[s, down(x), :] = acc[s, down(x), :] + (ring[s, 2] + ring[s, 5])
        st[s]["z"] = [copy(acc.at[(s,) + zpart(wz(z + d))], zb.at[s, d - 1], zs[d - 1]) for d in range(1, NZ)]

    def s4(s):
        for m in st[s]["z"]:
            m.wait_recv()
        r, l = zpart(z)
        t = acc[s, r, l]
        for d in range(NZ - 1):
            t = t + zb[s, d]
        t = t * scale
        zfin[s] = t
        r = rows_of(mine + x * pa + lax.div(z, 2) * zrow, zrow)
        st[s]["zz"] = [copy(zfin.at[s], fin.at[s, r, l], zs[d - 1]) for d in range(1, NZ)]
        fin[s, r, l] = t

    def s5(s):
        for m in st[s]["zz"]:
            m.wait_recv()
        f = lambda r: fin.at[s, r]
        fu = lambda q: f(rows_of(mine + q * pa, h))
        fd = lambda q: f(rows_of(mine + q * pa + h, h))
        st[s]["x"] = [
            copy(fu(x), fu(x), right), copy(fd(x), fd(x), left), copy(fd(x), fd(x), right), copy(fu(x), fu(x), left),
        ]
        whole = f(rows_of(mine + x * pa, pa))
        st[s]["o"] = [copy(whole, whole, other)]

    def s6(s):
        f = lambda r: fin.at[s, r]
        fu, fd = f(rows_of(mine + xb * pa, h)), f(rows_of(mine + xa * pa + h, h))
        m = st[s]["x"]
        m[0].wait_recv()
        m.append(copy(fu, fu, right))
        m[1].wait_recv()
        m.append(copy(fd, fd, left))

    def s7(s):
        m = st[s]["x"]
        m[2].wait_recv()
        m[3].wait_recv()
        for q in (xb, xa):
            whole = fin.at[s, rows_of(mine + q * pa, pa)]
            st[s]["o"].append(copy(whole, whole, other))
        m[4].wait_recv()
        m[5].wait_recv()
        whole = fin.at[s, rows_of(mine + xf * pa, pa)]
        st[s]["o"].append(copy(whole, whole, other))

    def s8(s):
        for m in st[s]["o"]:
            m.wait_recv()
        for i in range(2):
            to, frm = lanes_of(at[s][i], hp), pl.ds(i * hp, hp)
            block = fin[s, pl.ds(0, nq), frm]
            coeffs[:, to] = block
            ch[:, to], cl[:, to] = halves(block)
            pp[:, to] = fin[s, pl.ds(nq, npan), frm]

    rest = {}

    hq = hp // 4
    far_parts = {"a": [], "b": []}

    def far_sum(i):
        p = pl.ds(i * hq, hq)
        far_parts["a"].append(copy(s_ref.at[2, p], mid.at[0, p], north))
        far_parts["b"].append(copy(s_ref.at[2, pl.ds(hp + i * hq, hq)], mid.at[1, p], south))

    def near_sum():
        for m in far_parts["a"]:
            m.wait_recv()
        mid[6] = mid[0] + s_ref[3, pl.ds(hp, hp), :]
        rest["e"] = copy(mid.at[6], mid.at[4], north)
        for m in far_parts["b"]:
            m.wait_recv()
        mid[7] = mid[1] + s_ref[3, pl.ds(0, hp), :]
        rest["f"] = copy(mid.at[7], mid.at[5], south)

    def s9(s):
        t = dot3(halves(fin[s, pl.ds(0, nq), :]), (wh[pl.ds(0, nq)], wl[pl.ds(0, nq)]), TN)
        s_ref[s] = t
        lo, hi = s_ref.at[s, pl.ds(0, hp)], s_ref.at[s, pl.ds(hp, hp)]
        if s == 1:
            rest["c"] = copy(hi, mid.at[2], north)
            rest["d"] = copy(lo, mid.at[3], south)
        if s == 2:
            for i in range(3):
                far_sum(i)

    ng = part.shape[0]
    gq = ng // NY

    def g0():
        for u, rb in enumerate((x, 7 - x)):
            ct[...] = coeffs[:, lanes_of(rb * 128, 128)].T
            rs[pl.ds(u * 64, 64), pl.ds(0, nq)] = ct[rows_of(c * 64, 64), :]
        prod = dot3(halves(rs[:, pl.ds(0, nq)]), (ch[...], cl[...]), NN)
        rs[...] = prod
        for k in range(9):
            first = k < 8 - x
            rb = jnp.where(first, x, 7 - x)
            cb = jnp.where(first, x + k, k - 1)
            u = jnp.where(first, 0, 1)
            l = lanes_of(cb * 128, 128)
            own = (lax.div(rb, 2) == y).astype(F32)
            part[:, pl.ds(k * 128, 128)] = own * pp[rows_of(lax.rem(rb, 2) * 128 + c * 64, 64), l] - rs[rows_of(u * 64, 64), l]
        rest["r1"] = [copy(part.at[rows_of(wy(y + d) * gq, gq)], yb.at[d - 1], ys[d - 1]) for d in (2, 1, 3)]
        far_sum(3)

    gbase = c * (ng * NX)

    def g1():
        for m in rest["r1"]:
            m.wait_recv()
        t = part[rows_of(y * gq, gq)]
        for d in range(NY - 1):
            t = t + yb[d]
        gfin[...] = t
        to = rows_of(gbase + x * ng + y * gq, gq)
        rest["r2"] = [copy(gfin, g.at[to], ys[d - 1]) for d in (2, 1, 3)]
        g[to] = t
        near_sum()

    def summed():
        upper = lambda b: whole.at[rows_of(b * npan, hp)]
        lower = lambda b: whole.at[rows_of(b * npan + hp, hp)]
        same = lambda ref, to: plan(ref, ref, to)
        rest["d"].wait_recv()
        rest["e"].wait_recv()
        whole[rows_of(y * npan, hp)] = p_ref[pl.ds(0, hp)] - (s_ref[0, pl.ds(0, hp), :] + (mid[3] + mid[4]))
        early = [copy(upper(y), upper(y), north)]
        rest["c"].wait_recv()
        rest["f"].wait_recv()
        whole[rows_of(y * npan + hp, hp)] = p_ref[pl.ds(hp, hp)] - (s_ref[0, pl.ds(hp, hp), :] + (mid[2] + mid[5]))
        early.append(copy(lower(y), lower(y), south))
        rest["early"] = early
        rest["later"] = [copy(lower(y), lower(y), north), copy(upper(y), upper(y), south)]
        rest["pass_on"] = [same(upper(yb_), north), same(lower(ya), south)]

    def g2():
        for m in rest["r2"]:
            m.wait_recv()
        hg = ng // 2
        upper = lambda b: g.at[rows_of(gbase + b * ng, hg)]
        lower = lambda b: g.at[rows_of(gbase + b * ng + hg, hg)]
        whole_of = lambda b: g.at[rows_of(gbase + b * ng, ng)]
        m = [
            copy(upper(x), upper(x), right), copy(lower(x), lower(x), left),
            copy(lower(x), lower(x), right), copy(upper(x), upper(x), left),
        ]
        last = [copy(whole_of(x), whole_of(x), other)]
        m[0].wait_recv()
        m.append(copy(upper(xb), upper(xb), right))
        m[1].wait_recv()
        m.append(copy(lower(xa), lower(xa), left))
        m[2].wait_recv()
        last.append(copy(whole_of(xb), whole_of(xb), other))
        m[3].wait_recv()
        last.append(copy(whole_of(xa), whole_of(xa), other))
        m[4].wait_recv()
        m[5].wait_recv()
        last.append(copy(whole_of(xf), whole_of(xf), other))
        summed()
        for q in last:
            q.wait_recv()

    stages = (s0, s1, s2, s3, s4, s5, s6, s7, s8, s9)
    order = [(START[s] + AFTER[k], s, stages[k]) for s in range(4) for k in range(9)]
    order += [(START[s] + AFTER[8] + 0.1, s, s9) for s in (1, 2)]
    for _, s, stage in sorted(order, key=lambda e: e[:2]):
        stage(s)
    kept = pltpu.make_async_copy(coeffs, coeffs_hbm, done)
    kept.start()
    g0()
    s9(3)
    s9(0)
    g1()
    g2()
    def split(b):
        r = rows_of(b * npan, npan)
        rh[r, :], rl[r, :] = halves(whole[r, :])

    later, pass_on = rest["later"], rest["pass_on"]

    def passed():
        for i in range(2):
            rest["early"][i].wait_recv()
            pass_on[i].start()

    def near():
        split(y)
        for m in later:
            m.wait_recv()
        split(yb_)
        split(ya)

    factorize(g, m_ref, th, tl, dict(zip(HOOKS, (passed, near))))
    mine_rows = m_ref[rows_of(y * npan, npan), :]
    total = mine_rows.shape[1]
    row = lax.broadcasted_iota(jnp.int32, (npan, total), 0) + y * npan
    col = lax.broadcasted_iota(jnp.int32, (npan, total), 1)
    xh, xl = halves(jnp.where(col <= row, mine_rows, 0.0))
    ch[pl.ds(0, npan)], cl[pl.ds(0, npan)] = xh, xl
    for m in pass_on:
        m.wait_recv()
    split(yf)

    def columns(i, _):
        l = lanes_of(i * 256, 256)
        out[:, l] = dot3((ch[pl.ds(0, npan)], cl[pl.ds(0, npan)]), (rh[:, l], rl[:, l]), NN)
        return 0

    lax.fori_loop(0, out.shape[1] // 256, columns, 0)
    kept.wait()
    for m in made:
        m.wait_send()


HOOKS = (2, 5)
START = (3.0, 13.0, 27.0, 34.5)
AFTER = (0.0, 2.0, 5.0, 8.0, 15.0, 22.0, 25.0, 28.0, 32.0)


def step(basis, panel, scale):
    nq, w = basis.shape
    npan = panel.shape[0]
    total = npan * NY
    n = nq + npan
    half = n // 2
    pa = half // NX
    hp = npan // 2
    space = pl.BlockSpec(memory_space=pltpu.VMEM)
    short = [(n, w), (n, w), (nq, total), (nq, total)] + [(B, total + SPARE * B)] * 2 + [(total, w)] * 2
    shapes = [
        (6, hp, w), (4, n, 2 * hp), (4, half, 2 * hp), (4, half, 2 * hp), (4, 8, pa // 2, 2 * hp),
        (4, NZ - 1, pa * 2 // NZ, 128), (4, pa * 2 // NZ, 128), (4, n, 2 * hp),
        (npan, total), (128, nq), (128, total), (64, 9 * 128), (4, npan, w), (512, 9 * 128), (total + SPARE * B, total),
        (NY - 1, 64 // NY, 9 * 128), (64 // NY, 9 * 128), (8, hp, w), (total, w), (nq, total),
    ]
    copies = 6 + 4 * (1 + 6 + 7 + 7 + 6 + 4) + 36
    return pl.pallas_call(
        functools.partial(step_kernel, scale),
        name="step",
        out_shape=[jax.ShapeDtypeStruct((npan, w), F32), jax.ShapeDtypeStruct((nq, total), F32)],
        in_specs=[space] * 2,
        out_specs=[space, pl.BlockSpec(memory_space=pl.ANY)],
        scratch_shapes=[pltpu.VMEM(s_, BF16) for s_ in short] + [pltpu.VMEM(s_, F32) for s_ in shapes]
        + [pltpu.SemaphoreType.DMA((copies,)), pltpu.SemaphoreType.DMA((copies,)), pltpu.SemaphoreType.DMA(())],
        compiler_params=pltpu.CompilerParams(collective_id=1, has_side_effects=True, vmem_limit_bytes=60 * 2**20),
    )(basis, panel)


def body(basis, panel):
    n_grid = panel.shape[1] * lax.axis_size("grid")
    return tuple(step(basis, panel, 1.0 / n_grid))


def solution(mesh):
    placed = (P("band", "grid"), P("band", "grid"))
    return jax.shard_map(
        body, mesh=mesh, in_specs=placed, out_specs=(P("band", "grid"), P("band", None)), check_vma=False,
    )
```
